32 devices in a mesh: dp: 2 (over x), tp: 4 (over z), pp: 4 (over y, core).
Axes of the slice: x: 2, y: 2, z: 4, core: 2. Of those that a mesh axis runs over, the one named last changes fastest.
Arguments:
- x_micro: bfloat16 [16, 64, 1536], P('dp'), parts along dimension 0
- targets: bfloat16 [16, 64, 1536], P('dp'), parts along dimension 0
- w_in: bfloat16 [4, 2, 1536, 6144], P('pp', None, None, 'tp')
- w_out: bfloat16 [4, 2, 6144, 1536], P('pp', None, 'tp')
Outputs:
- output 1: float32 [8, 2, 1536, 6144], P(('dp', 'pp'), None, None, 'tp'), parts along dimension 0
- output 2: float32 [8, 2, 6144, 1536], P(('dp', 'pp'), None, 'tp'), parts along dimension 0
- output 3: float32 [2], P('dp'), parts along dimension 0
There are 2 independent parts. The reference program is written for one: setup_inputs(seed, part) draws one part's arguments, and reference() takes and returns one part's arrays. A program takes and returns all parts, laid end to end along the dimension named above; an argument that names none is the same for every part.
All inputs are finite; a program needn't handle non-finite values.
Results may differ from the reference program's by a relative error of at most 0.00675837.
Values are sent between devices in bfloat16 or wider.
A program may use at most 1 GiB of HBM per device.

```python
import jax
import jax.numpy as jnp
from jax import lax

N_MICRO = 8
N_STAGE = 4
N_TOKEN = 64
D_MODEL = 1536
D_FF = 6144


def setup_inputs(seed: int = 0, part: int = 0) -> dict:
    base_key = jax.random.key(seed)
    data_key = jax.random.fold_in(base_key, part)
    key_x, key_t = jax.random.split(data_key)
    key_first, key_second = jax.random.split(jax.random.key(seed + 1))
    x_micro = jax.random.normal(key_x, (N_MICRO, N_TOKEN, D_MODEL), jnp.float32)
    targets = jax.random.normal(key_t, (N_MICRO, N_TOKEN, D_MODEL), jnp.float32)
    w_in = jax.random.normal(key_first, (N_STAGE, 2, D_MODEL, D_FF), jnp.float32) * (D_MODEL ** -0.5)
    w_out = jax.random.normal(key_second, (N_STAGE, 2, D_FF, D_MODEL), jnp.float32) * (D_FF ** -0.5)
    return {'x_micro': x_micro.astype(jnp.bfloat16), 'targets': targets.astype(jnp.bfloat16), 'w_in': w_in.astype(jnp.bfloat16), 'w_out': w_out.astype(jnp.bfloat16)}


def gelu_fn(val):
    return jax.nn.gelu(val, approximate=True)


def layer_forward(h_in, w_first, w_second):
    pre_act = jnp.dot(h_in, w_first, preferred_element_type=jnp.float32).astype(jnp.bfloat16)
    hidden = gelu_fn(pre_act.astype(jnp.float32)).astype(jnp.bfloat16)
    branch = jnp.dot(hidden, w_second, preferred_element_type=jnp.float32)
    h_out = (h_in.astype(jnp.float32) + branch).astype(jnp.bfloat16)
    return h_out, pre_act


def layer_backward(grad_h, h_in, pre_act, w_first, w_second):
    grad_hidden = jnp.dot(grad_h, w_second.T, preferred_element_type=jnp.float32)
    hidden_f, pull_back = jax.vjp(gelu_fn, pre_act.astype(jnp.float32))
    grad_pre = pull_back(grad_hidden)[0].astype(jnp.bfloat16)
    branch = jnp.dot(grad_pre, w_first.T, preferred_element_type=jnp.float32)
    grad_in = (grad_h.astype(jnp.float32) + branch).astype(jnp.bfloat16)
    grad_second = jnp.dot(hidden_f.astype(jnp.bfloat16).T, grad_h, preferred_element_type=jnp.float32)
    grad_first = jnp.dot(h_in.T, grad_pre, preferred_element_type=jnp.float32)
    return grad_in, grad_first, grad_second


def reference(x_micro, targets, w_in, w_out):
    n_layer = 2 * N_STAGE
    w_first = w_in.reshape(n_layer, D_MODEL, D_FF)
    w_second = w_out.reshape(n_layer, D_FF, D_MODEL)
    norm_factor = 1.0 / (N_MICRO * N_TOKEN * D_MODEL)

    def fwd_step(h_cur, weights):
        h_next, pre_act = layer_forward(h_cur, weights[0], weights[1])
        return h_next, (h_cur, pre_act)

    def bwd_step(grad_h, saved):
        grad_in, grad_first, grad_second = layer_backward(grad_h, saved[0], saved[1], saved[2], saved[3])
        return grad_in, (grad_first, grad_second)

    def micro_step(carry, batch):
        loss_sum, acc_first, acc_second = carry
        y_out, (h_ins, pre_acts) = lax.scan(fwd_step, batch[0], (w_first, w_second))
        mismatch = y_out.astype(jnp.float32) - batch[1].astype(jnp.float32)
        loss_sum = loss_sum + 0.5 * jnp.sum(mismatch * mismatch)
        grad_y = (mismatch * norm_factor).astype(jnp.bfloat16)
        _, (grad_first, grad_second) = lax.scan(bwd_step, grad_y, (h_ins, pre_acts, w_first, w_second), reverse=True)
        return (loss_sum, acc_first + grad_first, acc_second + grad_second), None

    init_carry = (jnp.zeros((), jnp.float32), jnp.zeros((n_layer, D_MODEL, D_FF), jnp.float32), jnp.zeros((n_layer, D_FF, D_MODEL), jnp.float32))
    (loss_sum, acc_first, acc_second), _ = lax.scan(micro_step, init_carry, (x_micro, targets))
    return (acc_first.reshape(N_STAGE, 2, D_MODEL, D_FF), acc_second.reshape(N_STAGE, 2, D_FF, D_MODEL), (loss_sum * norm_factor).reshape(1))
```

```python
import functools
import math

import jax
import jax.numpy as jnp
from jax import lax
from jax.experimental import pallas as pl
from jax.experimental.pallas import tpu as pltpu
from jax.sharding import PartitionSpec as P

UNIT = 32
N_CHUNK = 2
SLOTS = 4
BLOCK = 512

MESH = pl.DeviceIdType.MESH
F32 = jnp.float32
BF16 = jnp.bfloat16
ROOT = math.sqrt(2 / math.pi)
CUBIC = 0.044715


def gelu_parts(val):
    th = jnp.tanh(ROOT * (val + CUBIC * (val * val * val)))
    cdf = 0.5 * (1.0 + th)
    return val * cdf, cdf + val * (0.5 * (1.0 - th * th) * (ROOT * (1.0 + 3.0 * CUBIC * (val * val))))


def gelu_only(val):
    return val * (0.5 * (1.0 + jnp.tanh(ROOT * (val + CUBIC * (val * val * val)))))


def dot_nn(a, b):
    return jnp.dot(a, b, preferred_element_type=F32)


def dot_nt(a, b):
    return lax.dot_general(a, b, (((1,), (1,)), ((), ())), preferred_element_type=F32)


def pipe_kernel(norm, x_hbm, t_hbm, w1_hbm, w2_hbm,
                h_out, g_out, a_out, e_out, loss_out,
                w1, w2, xs, us, acts, tgt, act_now, part, recv, outb, loss_acc, loss_src, loss_dst,
                w_sem, in_sem, x_sem, part_sem, recv_sem, leaf_sem, peer_sem, copy_sem, loss_sem, loss_got):
    n_stage, n_tp = 4, 4
    _, n, unit, width = xs.shape
    hid = us.shape[3]
    cw = width // N_CHUNK
    stage = lax.axis_index('pp')
    z = lax.axis_index('tp')
    last = n_stage - 1
    is_center = (z == 1) | (z == 2)
    is_leaf = (z == 0) | (z == 3)
    center_i = is_center.astype(jnp.int32)
    partner = z + 1 - 2 * (z % 2)
    peer = partner + center_i * (3 - z - partner)
    at_last_i = (stage == last).astype(jnp.int32)
    gap = 2 - 2 * at_last_i

    w_copies = []
    for k in range(2):
        w_copies.append((pltpu.make_async_copy(w1_hbm.at[k], w1.at[k], w_sem.at[0, k]),
                         pltpu.make_async_copy(w2_hbm.at[k], w2.at[k], w_sem.at[1, k])))
    x_copy = pltpu.make_async_copy(x_hbm, xs.at[0], in_sem.at[0])
    t_copy = pltpu.make_async_copy(t_hbm, tgt, in_sem.at[1])

    @pl.when(stage == 0)
    def _():
        x_copy.start()

    for pair in w_copies:
        for copy in pair:
            copy.start()
    t_copy.start()
    loss_acc[...] = jnp.zeros_like(loss_acc)

    barrier = pltpu.get_barrier_semaphore()
    for ds in range(n_stage):
        for dz in range(n_tp):
            if ds or dz:
                pl.semaphore_signal(barrier, inc=1, device_id={'pp': (stage + ds) % n_stage, 'tp': (z + dz) % n_tp}, device_id_type=MESH)
    pl.semaphore_wait(barrier, n_stage * n_tp - 1)

    @pl.when(stage == 0)
    def _():
        x_copy.wait()

    t_copy.wait()

    def cols(c):
        return pl.ds(c * cw, cw)

    def part_send(p, slot, c):
        return pltpu.make_async_remote_copy(
            src_ref=part.at[p, slot, c], dst_ref=recv.at[center_i, p, slot, c],
            send_sem=part_sem.at[p, slot, c], recv_sem=recv_sem.at[center_i, p, slot, c],
            device_id={'pp': stage, 'tp': peer}, device_id_type=MESH)

    def part_arrival(kind, p, slot, c):
        return pltpu.make_async_remote_copy(
            src_ref=part.at[p, slot, c], dst_ref=recv.at[kind, p, slot, c],
            send_sem=part_sem.at[p, slot, c], recv_sem=recv_sem.at[kind, p, slot, c],
            device_id={'pp': stage, 'tp': peer}, device_id_type=MESH)

    def out_send(p, slot, c, q, m, to_stage, to_tp, sem):
        return pltpu.make_async_remote_copy(
            src_ref=outb.at[p, slot, c], dst_ref=xs.at[q, m, :, cols(c)],
            send_sem=sem.at[p, slot, c], recv_sem=x_sem.at[q, m, c],
            device_id={'pp': to_stage, 'tp': to_tp}, device_id_type=MESH)

    def at(v):
        fwd = (v >= 0) & (v < n)
        bwd = (v >= n + gap) & (v < 2 * n + gap)
        bwd_i = (v >= n).astype(jnp.int32)
        m = v - bwd_i * (n + gap)
        return fwd, bwd, bwd_i, m, m + bwd_i * n

    def arrived(q, m):
        for c in range(N_CHUNK):
            out_send(0, 0, c, q, m, stage, z, leaf_sem).wait_recv()

    def free_part(p, i):
        @pl.when(i >= SLOTS)
        def _():
            for c in range(N_CHUNK):
                part_send(p, i % SLOTS, c).wait_send()

    def send_part(p, slot, c):
        @pl.when(is_leaf)
        def _():
            part_send(p, slot, c).start()

    def compute(v, p):
        fwd, bwd, _, m, i = at(v)
        slot = i % SLOTS

        @pl.when(fwd)
        def _():
            @pl.when(m == 0)
            def _():
                w_copies[p][0].wait()
            if p == 0:
                @pl.when(stage > 0)
                def _():
                    arrived(0, m)
            else:
                @pl.when(is_leaf)
                def _():
                    arrived(1, m)
            free_part(p, i)
            for j in range(hid // BLOCK):
                js = pl.ds(j * BLOCK, BLOCK)
                pre = dot_nn(xs[p, m], w1[p, :, js]).astype(BF16)
                us[p, m, :, js] = pre
                act_now[:, js] = gelu_only(pre.astype(F32)).astype(BF16)

            @pl.when(m == 0)
            def _():
                w_copies[p][1].wait()
            for c in range(N_CHUNK):
                part[p, slot, c] = dot_nn(act_now[...], w2[p, :, cols(c)])
                send_part(p, slot, c)

        @pl.when(bwd)
        def _():
            k = 1 - p
            if p == 0:
                @pl.when(is_leaf | (stage < last))
                def _():
                    arrived(2, m)
            else:
                @pl.when(is_leaf)
                def _():
                    arrived(3, m)

            def outs():
                return (pltpu.make_async_copy(xs.at[k, m], h_out.at[k, m], copy_sem.at[p, 0]),
                        pltpu.make_async_copy(xs.at[2 + p, m], g_out.at[k, m], copy_sem.at[p, 1]),
                        pltpu.make_async_copy(acts.at[k, m], a_out.at[k, m], copy_sem.at[p, 2]),
                        pltpu.make_async_copy(us.at[k, m], e_out.at[k, m], copy_sem.at[p, 3]))

            @pl.when(m > 0)
            def _():
                for copy in outs():
                    copy.wait()
            for j in range(hid // BLOCK):
                js = pl.ds(j * BLOCK, BLOCK)
                grad = dot_nt(xs[2 + p, m], w2[k, js, :])
                act, slope = gelu_parts(us[k, m, :, js].astype(F32))
                acts[k, m, :, js] = act.astype(BF16)
                err = (slope * grad).astype(BF16)
                us[k, m, :, js] = err
                act_now[:, js] = err

            def down():
                free_part(p, i)
                for c in range(N_CHUNK):
                    part[p, slot, c] = dot_nt(act_now[...], w1[k, cols(c), :])
                    send_part(p, slot, c)

            if p == 0:
                down()
            else:
                pl.when(stage > 0)(down)
            for copy in outs():
                copy.start()

    def sums(v, p):
        fwd, bwd, bwd_i, m, i = at(v)
        live = fwd | bwd if p == 0 else fwd | (bwd & (stage > 0))
        return live & is_center, fwd, bwd_i, m, i, i % SLOTS

    def add_leaf(v, p):
        live, _, _, _, _, slot = sums(v, p)

        @pl.when(live)
        def _():
            for c in range(N_CHUNK):
                part_arrival(0, p, slot, c).wait_recv()
                part[p, slot, c] = part[p, slot, c] + recv[0, p, slot, c]
                part_send(p, slot, c).start()

    def finish(v, p):
        live, fwd, bwd_i, m, i, slot = sums(v, p)
        if p == 0:
            to_stage, q = stage, 1 + 2 * bwd_i
        else:
            home = (1 - bwd_i) * at_last_i
            to_stage, q = stage + (1 - home) * (1 - 2 * bwd_i), 2 * bwd_i + 2 * home

        @pl.when(live)
        def _():
            @pl.when(i >= SLOTS)
            def _():
                for c in range(N_CHUNK):
                    out_send(p, slot, c, q, m, to_stage, partner, leaf_sem).wait_send()
            if p == 1:
                @pl.when((i >= SLOTS) & ((stage < last) | (i >= SLOTS + n)))
                def _():
                    for c in range(N_CHUNK):
                        out_send(p, slot, c, q, m, to_stage, z, peer_sem).wait_send()
            for c in range(N_CHUNK):
                part_arrival(1, p, slot, c).wait_recv()
                res = (xs[2 * bwd_i + p, m, :, cols(c)].astype(F32) + (part[p, slot, c] + recv[1, p, slot, c])).astype(BF16)
                if p == 0:
                    outb[p, slot, c] = res
                    xs[q, m, :, cols(c)] = res
                else:
                    @pl.when((stage < last) | (bwd_i == 1))
                    def _():
                        outb[p, slot, c] = res
                        out_send(p, slot, c, q, m, to_stage, z, peer_sem).start()

                    @pl.when((stage == last) & (bwd_i == 0))
                    def _():
                        diff = res.astype(F32) - tgt[m, :, cols(c)].astype(F32)
                        grad = (diff * norm).astype(BF16)
                        outb[p, slot, c] = grad
                        xs[q, m, :, cols(c)] = grad
                        sq = diff * diff
                        acc = loss_acc[...]
                        for r in range(unit // 8):
                            for b in range(cw // 128):
                                acc = acc + sq[r * 8:(r + 1) * 8, b * 128:(b + 1) * 128]
                        loss_acc[...] = acc
                out_send(p, slot, c, q, m, to_stage, partner, leaf_sem).start()

    def step(t, carry):
        compute(t, 0)
        add_leaf(t - 2, 1)
        finish(t - 1, 0)
        compute(t - 1, 1)
        add_leaf(t, 0)
        finish(t - 2, 1)
        return carry

    lax.fori_loop(0, 2 * n + 4, step, 0)

    for p in range(2):
        for slot in range(SLOTS):
            for c in range(N_CHUNK):
                part_send(p, slot, c).wait_send()

                @pl.when(is_center)
                def _():
                    out_send(p, slot, c, 0, 0, stage, partner, leaf_sem).wait_send()
                    if p == 1:
                        out_send(p, slot, c, 0, 0, stage, z, peer_sem).wait_send()
        k = 1 - p
        pltpu.make_async_copy(xs.at[k, 0], h_out.at[k, 0], copy_sem.at[p, 0]).wait()
        pltpu.make_async_copy(xs.at[2 + p, 0], g_out.at[k, 0], copy_sem.at[p, 1]).wait()
        pltpu.make_async_copy(acts.at[k, 0], a_out.at[k, 0], copy_sem.at[p, 2]).wait()
        pltpu.make_async_copy(us.at[k, 0], e_out.at[k, 0], copy_sem.at[p, 3]).wait()

    def loss_send(idx, to_stage, to_tp):
        return pltpu.make_async_remote_copy(
            src_ref=loss_src, dst_ref=loss_dst, send_sem=loss_sem.at[idx], recv_sem=loss_got.at[0],
            device_id={'pp': to_stage, 'tp': to_tp}, device_id_type=MESH)

    sender = is_center & (stage == last)

    @pl.when(sender)
    def _():
        total = jnp.sum(loss_acc[...]) * 0.5 * norm
        value = jnp.full(loss_src.shape, total, F32)
        loss_src[...] = value
        loss_out[...] = value
        sends = [loss_send(2 * s + b, s, z if b else partner) for s in range(n_stage) for b in range(2) if not (s == last and b)]
        for send in sends:
            send.start()
        for send in sends:
            send.wait_send()

    @pl.when(is_leaf | (stage < last))
    def _():
        loss_send(0, stage, z).wait_recv()
        loss_out[...] = loss_dst[...]


def solution(mesh):
    def stage_body(x_micro, targets, w_in, w_out):
        n_micro, n_token, width = x_micro.shape
        hid = w_in.shape[3]
        n = n_micro * n_token // UNIT
        norm = 1.0 / (n_micro * n_token * width)
        cw = width // N_CHUNK
        any_spec = pl.BlockSpec(memory_space=pl.ANY)
        h, g, a, e, loss = pl.pallas_call(
            functools.partial(pipe_kernel, norm),
            out_shape=(
                jax.ShapeDtypeStruct((2, n, UNIT, width), BF16),
                jax.ShapeDtypeStruct((2, n, UNIT, width), BF16),
                jax.ShapeDtypeStruct((2, n, UNIT, hid), BF16),
                jax.ShapeDtypeStruct((2, n, UNIT, hid), BF16),
                jax.ShapeDtypeStruct((8, 128), F32),
            ),
            in_specs=[any_spec] * 4,
            out_specs=(any_spec, any_spec, any_spec, any_spec, pl.BlockSpec(memory_space=pltpu.VMEM)),
            scratch_shapes=[
                pltpu.VMEM((2, width, hid), BF16),
                pltpu.VMEM((2, hid, width), BF16),
                pltpu.VMEM((4, n, UNIT, width), BF16),
                pltpu.VMEM((2, n, UNIT, hid), BF16),
                pltpu.VMEM((2, n, UNIT, hid), BF16),
                pltpu.VMEM((n, UNIT, width), BF16),
                pltpu.VMEM((UNIT, hid), BF16),
                pltpu.VMEM((2, SLOTS, N_CHUNK, UNIT, cw), F32),
                pltpu.VMEM((2, 2, SLOTS, N_CHUNK, UNIT, cw), F32),
                pltpu.VMEM((2, SLOTS, N_CHUNK, UNIT, cw), BF16),
                pltpu.VMEM((8, 128), F32),
                pltpu.VMEM((8, 128), F32),
                pltpu.VMEM((8, 128), F32),
                pltpu.SemaphoreType.DMA((2, 2)),
                pltpu.SemaphoreType.DMA((2,)),
                pltpu.SemaphoreType.DMA((4, n, N_CHUNK)),
                pltpu.SemaphoreType.DMA((2, SLOTS, N_CHUNK)),
                pltpu.SemaphoreType.DMA((2, 2, SLOTS, N_CHUNK)),
                pltpu.SemaphoreType.DMA((2, SLOTS, N_CHUNK)),
                pltpu.SemaphoreType.DMA((2, SLOTS, N_CHUNK)),
                pltpu.SemaphoreType.DMA((2, 4)),
                pltpu.SemaphoreType.DMA((8,)),
                pltpu.SemaphoreType.DMA((1,)),
            ],
            compiler_params=pltpu.CompilerParams(collective_id=0, has_side_effects=True, vmem_limit_bytes=60 * 1024 * 1024),
        )(x_micro.reshape(n, UNIT, width), targets.reshape(n, UNIT, width), w_in[0], w_out[0])

        h, g = (v.reshape(2, n * UNIT, width) for v in (h, g))
        a, e = (v.reshape(2, n * UNIT, hid) for v in (a, e))
        grad_first = jnp.einsum('kbd,kbf->kdf', h, e, preferred_element_type=F32)
        grad_second = jnp.einsum('kbf,kbd->kfd', a, g, preferred_element_type=F32)
        return grad_first[None], grad_second[None], loss[0, :1]

    data_spec = P('dp', None, None)
    return jax.shard_map(stage_body, mesh=mesh, in_specs=(data_spec, data_spec, P('pp', None, None, 'tp'), P('pp', None, 'tp', None)), out_specs=(P(('dp', 'pp'), None, None, 'tp'), P(('dp', 'pp'), None, 'tp', None), P('dp')), check_vma=False)
```

```python
import functools
import math

import jax
import jax.numpy as jnp
from jax import lax
from jax.experimental import pallas as pl
from jax.experimental.pallas import tpu as pltpu
from jax.sharding import PartitionSpec as P

UNIT = 32
N_CHUNK = 3
SLOTS = 4
BLOCK = 512
GAP = 3

MESH = pl.DeviceIdType.MESH
F32 = jnp.float32
BF16 = jnp.bfloat16
ROOT = math.sqrt(2 / math.pi)
CUBIC = 0.044715


def gelu_parts(val):
    th = jnp.tanh(ROOT * (val + CUBIC * (val * val * val)))
    cdf = 0.5 * (1.0 + th)
    return val * cdf, cdf + val * (0.5 * (1.0 - th * th) * (ROOT * (1.0 + 3.0 * CUBIC * (val * val))))


def gelu_only(val):
    return val * (0.5 * (1.0 + jnp.tanh(ROOT * (val + CUBIC * (val * val * val)))))


def dot_nn(a, b):
    return jnp.dot(a, b, preferred_element_type=F32)


def dot_nt(a, b):
    return lax.dot_general(a, b, (((1,), (1,)), ((), ())), preferred_element_type=F32)


def pipe_kernel(norm, x_hbm, t_hbm, w1_hbm, w2_hbm,
                h_out, g_out, a_out, e_out, loss_out,
                w1, w2, xs, us, acts, tgt, act_now, part, recv, outb, loss_acc, loss_src, loss_dst,
                w_sem, in_sem, x_sem, part_sem, recv_sem, leaf_sem, peer_sem, copy_sem, loss_sem, loss_got):
    n_stage, n_tp = 4, 4
    _, n, unit, width = xs.shape
    hid = us.shape[3]
    cw = width // N_CHUNK
    stage = lax.axis_index('pp')
    z = lax.axis_index('tp')
    last = n_stage - 1
    is_center = (z == 1) | (z == 2)
    is_leaf = (z == 0) | (z == 3)
    center_i = is_center.astype(jnp.int32)
    partner = z + 1 - 2 * (z % 2)
    peer = partner + center_i * (3 - z - partner)
    at_last_i = (stage == last).astype(jnp.int32)
    gap = GAP * (1 - at_last_i)

    w_copies = []
    for k in range(2):
        w_copies.append((pltpu.make_async_copy(w1_hbm.at[k], w1.at[k], w_sem.at[0, k]),
                         pltpu.make_async_copy(w2_hbm.at[k], w2.at[k], w_sem.at[1, k])))
    x_copy = pltpu.make_async_copy(x_hbm, xs.at[0], in_sem.at[0])
    t_copy = pltpu.make_async_copy(t_hbm, tgt, in_sem.at[1])

    @pl.when(stage == 0)
    def _():
        x_copy.start()

    for pair in w_copies:
        for copy in pair:
            copy.start()
    t_copy.start()
    loss_acc[...] = jnp.zeros_like(loss_acc)

    barrier = pltpu.get_barrier_semaphore()
    for ds in range(n_stage):
        for dz in range(n_tp):
            if ds or dz:
                pl.semaphore_signal(barrier, inc=1, device_id={'pp': (stage + ds) % n_stage, 'tp': (z + dz) % n_tp}, device_id_type=MESH)
    pl.semaphore_wait(barrier, n_stage * n_tp - 1)

    @pl.when(stage == 0)
    def _():
        x_copy.wait()

    @pl.when(stage == last)
    def _():
        t_copy.wait()

    def cols(c):
        return pl.ds(c * cw, cw)

    def part_send(p, slot, c):
        return pltpu.make_async_remote_copy(
            src_ref=part.at[p, slot, c], dst_ref=recv.at[center_i, p, slot, c],
            send_sem=part_sem.at[p, slot, c], recv_sem=recv_sem.at[center_i, p, slot, c],
            device_id={'pp': stage, 'tp': peer}, device_id_type=MESH)

    def part_arrival(kind, p, slot, c):
        return pltpu.make_async_remote_copy(
            src_ref=part.at[p, slot, c], dst_ref=recv.at[kind, p, slot, c],
            send_sem=part_sem.at[p, slot, c], recv_sem=recv_sem.at[kind, p, slot, c],
            device_id={'pp': stage, 'tp': peer}, device_id_type=MESH)

    def out_send(p, slot, c, q, m, to_stage, to_tp, sem):
        return pltpu.make_async_remote_copy(
            src_ref=outb.at[p, slot, c], dst_ref=xs.at[q, m, :, cols(c)],
            send_sem=sem.at[p, slot, c], recv_sem=x_sem.at[q, m, c],
            device_id={'pp': to_stage, 'tp': to_tp}, device_id_type=MESH)

    def at(v):
        fwd = (v >= 0) & (v < n)
        bwd = (v >= n + gap) & (v < 2 * n + gap)
        bwd_i = (v >= n).astype(jnp.int32)
        m = v - bwd_i * (n + gap)
        return fwd, bwd, bwd_i, m, m + bwd_i * n

    def arrived(q, m):
        for c in range(N_CHUNK):
            out_send(0, 0, c, q, m, stage, z, leaf_sem).wait_recv()

    def free_part(p, i):
        @pl.when(i >= SLOTS)
        def _():
            for c in range(N_CHUNK):
                part_send(p, i % SLOTS, c).wait_send()

    def send_part(p, slot, c):
        @pl.when(is_leaf)
        def _():
            part_send(p, slot, c).start()

    def compute(v, p):
        fwd, bwd, _, m, i = at(v)
        slot = i % SLOTS

        @pl.when(fwd)
        def _():
            @pl.when(m == 0)
            def _():
                w_copies[p][0].wait()
            if p == 0:
                @pl.when(stage > 0)
                def _():
                    arrived(0, m)
            else:
                @pl.when(is_leaf)
                def _():
                    arrived(1, m)
            free_part(p, i)
            for j in range(hid // BLOCK):
                js = pl.ds(j * BLOCK, BLOCK)
                pre = dot_nn(xs[p, m], w1[p, :, js]).astype(BF16)
                us[p, m, :, js] = pre
                act_now[:, js] = gelu_only(pre.astype(F32)).astype(BF16)

            @pl.when(m == 0)
            def _():
                w_copies[p][1].wait()
            for c in range(N_CHUNK):
                part[p, slot, c] = dot_nn(act_now[...], w2[p, :, cols(c)])
                send_part(p, slot, c)

        @pl.when(bwd)
        def _():
            k = 1 - p
            if p == 0:
                @pl.when(is_leaf | (stage < last))
                def _():
                    arrived(2, m)
            else:
                @pl.when(is_leaf)
                def _():
                    arrived(3, m)

            def outs():
                return (pltpu.make_async_copy(xs.at[k, m], h_out.at[k, m], copy_sem.at[p, 0]),
                        pltpu.make_async_copy(xs.at[2 + p, m], g_out.at[k, m], copy_sem.at[p, 1]),
                        pltpu.make_async_copy(acts.at[k, m], a_out.at[k, m], copy_sem.at[p, 2]),
                        pltpu.make_async_copy(us.at[k, m], e_out.at[k, m], copy_sem.at[p, 3]))

            @pl.when(m > 0)
            def _():
                for copy in outs():
                    copy.wait()
            for j in range(hid // BLOCK):
                js = pl.ds(j * BLOCK, BLOCK)
                grad = dot_nt(xs[2 + p, m], w2[k, js, :])
                act, slope = gelu_parts(us[k, m, :, js].astype(F32))
                acts[k, m, :, js] = act.astype(BF16)
                err = (slope * grad).astype(BF16)
                us[k, m, :, js] = err
                act_now[:, js] = err

            def down():
                free_part(p, i)
                for c in range(N_CHUNK):
                    part[p, slot, c] = dot_nt(act_now[...], w1[k, cols(c), :])
                    send_part(p, slot, c)

            if p == 0:
                down()
            else:
                pl.when(stage > 0)(down)
            for copy in outs():
                copy.start()

    def sums(v, p):
        fwd, bwd, bwd_i, m, i = at(v)
        live = fwd | bwd if p == 0 else fwd | (bwd & (stage > 0))
        return live & is_center, fwd, bwd_i, m, i, i % SLOTS

    def add_leaf(v, p):
        live, _, _, _, _, slot = sums(v, p)

        @pl.when(live)
        def _():
            for c in range(N_CHUNK):
                part_arrival(0, p, slot, c).wait_recv()
                part[p, slot, c] = part[p, slot, c] + recv[0, p, slot, c]
                part_send(p, slot, c).start()

    def finish(v, p):
        live, fwd, bwd_i, m, i, slot = sums(v, p)
        if p == 0:
            to_stage, q = stage, 1 + 2 * bwd_i
        else:
            home = (1 - bwd_i) * at_last_i
            to_stage, q = stage + (1 - home) * (1 - 2 * bwd_i), 2 * bwd_i + 2 * home

        @pl.when(live)
        def _():
            @pl.when(i >= SLOTS)
            def _():
                for c in range(N_CHUNK):
                    out_send(p, slot, c, q, m, to_stage, partner, leaf_sem).wait_send()
            if p == 1:
                @pl.when((i >= SLOTS) & ((stage < last) | (i >= SLOTS + n)))
                def _():
                    for c in range(N_CHUNK):
                        out_send(p, slot, c, q, m, to_stage, z, peer_sem).wait_send()
            for c in range(N_CHUNK):
                part_arrival(1, p, slot, c).wait_recv()
                res = (xs[2 * bwd_i + p, m, :, cols(c)].astype(F32) + (part[p, slot, c] + recv[1, p, slot, c])).astype(BF16)
                if p == 0:
                    outb[p, slot, c] = res
                    xs[q, m, :, cols(c)] = res
                else:
                    @pl.when((stage < last) | (bwd_i == 1))
                    def _():
                        outb[p, slot, c] = res
                        out_send(p, slot, c, q, m, to_stage, z, peer_sem).start()

                    @pl.when((stage == last) & (bwd_i == 0))
                    def _():
                        diff = res.astype(F32) - tgt[m, :, cols(c)].astype(F32)
                        grad = (diff * norm).astype(BF16)
                        outb[p, slot, c] = grad
                        xs[q, m, :, cols(c)] = grad
                        sq = diff * diff
                        acc = loss_acc[...]
                        for r in range(unit // 8):
                            for b in range(cw // 128):
                                acc = acc + sq[r * 8:(r + 1) * 8, b * 128:(b + 1) * 128]
                        loss_acc[...] = acc
                out_send(p, slot, c, q, m, to_stage, partner, leaf_sem).start()

    def step(t, carry):
        compute(t - 3 + center_i, 1)
        compute(t, 0)
        finish(t - 1, 0)
        add_leaf(t, 0)
        finish(t - 3, 1)
        add_leaf(t - 2, 1)
        return carry

    lax.fori_loop(0, 2 * n + GAP + 3, step, 0)

    @pl.when(stage < last)
    def _():
        t_copy.wait()

    for p in range(2):
        for slot in range(SLOTS):
            for c in range(N_CHUNK):
                part_send(p, slot, c).wait_send()

                @pl.when(is_center)
                def _():
                    out_send(p, slot, c, 0, 0, stage, partner, leaf_sem).wait_send()
                    if p == 1:
                        out_send(p, slot, c, 0, 0, stage, z, peer_sem).wait_send()
        k = 1 - p
        pltpu.make_async_copy(xs.at[k, 0], h_out.at[k, 0], copy_sem.at[p, 0]).wait()
        pltpu.make_async_copy(xs.at[2 + p, 0], g_out.at[k, 0], copy_sem.at[p, 1]).wait()
        pltpu.make_async_copy(acts.at[k, 0], a_out.at[k, 0], copy_sem.at[p, 2]).wait()
        pltpu.make_async_copy(us.at[k, 0], e_out.at[k, 0], copy_sem.at[p, 3]).wait()

    def loss_send(idx, to_stage, to_tp):
        return pltpu.make_async_remote_copy(
            src_ref=loss_src, dst_ref=loss_dst, send_sem=loss_sem.at[idx], recv_sem=loss_got.at[0],
            device_id={'pp': to_stage, 'tp': to_tp}, device_id_type=MESH)

    sender = is_center & (stage == last)

    @pl.when(sender)
    def _():
        total = jnp.sum(loss_acc[...]) * 0.5 * norm
        value = jnp.full(loss_src.shape, total, F32)
        loss_src[...] = value
        loss_out[...] = value
        sends = [loss_send(2 * s + b, s, z if b else partner) for s in range(n_stage) for b in range(2) if not (s == last and b)]
        for send in sends:
            send.start()
        for send in sends:
            send.wait_send()

    @pl.when(is_leaf | (stage < last))
    def _():
        loss_send(0, stage, z).wait_recv()
        loss_out[...] = loss_dst[...]


def solution(mesh):
    def stage_body(x_micro, targets, w_in, w_out):
        n_micro, n_token, width = x_micro.shape
        hid = w_in.shape[3]
        n = n_micro * n_token // UNIT
        norm = 1.0 / (n_micro * n_token * width)
        cw = width // N_CHUNK
        any_spec = pl.BlockSpec(memory_space=pl.ANY)
        h, g, a, e, loss = pl.pallas_call(
            functools.partial(pipe_kernel, norm),
            out_shape=(
                jax.ShapeDtypeStruct((2, n, UNIT, width), BF16),
                jax.ShapeDtypeStruct((2, n, UNIT, width), BF16),
                jax.ShapeDtypeStruct((2, n, UNIT, hid), BF16),
                jax.ShapeDtypeStruct((2, n, UNIT, hid), BF16),
                jax.ShapeDtypeStruct((8, 128), F32),
            ),
            in_specs=[any_spec] * 4,
            out_specs=(any_spec, any_spec, any_spec, any_spec, pl.BlockSpec(memory_space=pltpu.VMEM)),
            scratch_shapes=[
                pltpu.VMEM((2, width, hid), BF16),
                pltpu.VMEM((2, hid, width), BF16),
                pltpu.VMEM((4, n, UNIT, width), BF16),
                pltpu.VMEM((2, n, UNIT, hid), BF16),
                pltpu.VMEM((2, n, UNIT, hid), BF16),
                pltpu.VMEM((n, UNIT, width), BF16),
                pltpu.VMEM((UNIT, hid), BF16),
                pltpu.VMEM((2, SLOTS, N_CHUNK, UNIT, cw), F32),
                pltpu.VMEM((2, 2, SLOTS, N_CHUNK, UNIT, cw), F32),
                pltpu.VMEM((2, SLOTS, N_CHUNK, UNIT, cw), BF16),
                pltpu.VMEM((8, 128), F32),
                pltpu.VMEM((8, 128), F32),
                pltpu.VMEM((8, 128), F32),
                pltpu.SemaphoreType.DMA((2, 2)),
                pltpu.SemaphoreType.DMA((2,)),
                pltpu.SemaphoreType.DMA((4, n, N_CHUNK)),
                pltpu.SemaphoreType.DMA((2, SLOTS, N_CHUNK)),
                pltpu.SemaphoreType.DMA((2, 2, SLOTS, N_CHUNK)),
                pltpu.SemaphoreType.DMA((2, SLOTS, N_CHUNK)),
                pltpu.SemaphoreType.DMA((2, SLOTS, N_CHUNK)),
                pltpu.SemaphoreType.DMA((2, 4)),
                pltpu.SemaphoreType.DMA((8,)),
                pltpu.SemaphoreType.DMA((1,)),
            ],
            compiler_params=pltpu.CompilerParams(collective_id=0, has_side_effects=True, vmem_limit_bytes=60 * 1024 * 1024),
        )(x_micro.reshape(n, UNIT, width), targets.reshape(n, UNIT, width), w_in[0], w_out[0])

        h, g = (v.reshape(2, n * UNIT, width) for v in (h, g))
        a, e = (v.reshape(2, n * UNIT, hid) for v in (a, e))
        grad_first = jnp.einsum('kbd,kbf->kdf', h, e, preferred_element_type=F32)
        grad_second = jnp.einsum('kbf,kbd->kfd', a, g, preferred_element_type=F32)
        return grad_first[None], grad_second[None], loss[0, :1]

    data_spec = P('dp', None, None)
    return jax.shard_map(stage_body, mesh=mesh, in_specs=(data_spec, data_spec, P('pp', None, None, 'tp'), P('pp', None, 'tp', None)), out_specs=(P(('dp', 'pp'), None, None, 'tp'), P(('dp', 'pp'), None, 'tp', None), P('dp')), check_vma=False)
```

```python
import functools
import math

import jax
import jax.numpy as jnp
from jax import lax
from jax.experimental import pallas as pl
from jax.experimental.pallas import tpu as pltpu
from jax.sharding import PartitionSpec as P

UNIT = 32
N_CHUNK = 3
SLOTS = 4
BLOCK = 512
TILE = 256
GAP = 4

MESH = pl.DeviceIdType.MESH
F32 = jnp.float32
BF16 = jnp.bfloat16
ROOT = math.sqrt(2 / math.pi)
CUBIC = 0.044715


ALL = tuple(range(N_CHUNK))
ORDER = (('sum', 3, 1, (1,)), ('dot', 0, 0, ALL), ('sum', 3, 1, (2,)), ('end', 1, 0, (1, 0)), ('sum', 0, 0, (0, 1)), ('end', 1, 0, (2,)),
         ('dot', 1, 1, ALL), ('end', 3, 1, (0,)), ('sum', 0, 0, (2,)), ('end', 3, 1, (1,)), ('sum', 2, 1, (0,)), ('end', 3, 1, (2,)))
OUTER_LAG = 2


def gelu_parts(val):
    th = jnp.tanh(ROOT * (val + CUBIC * (val * val * val)))
    cdf = 0.5 * (1.0 + th)
    return val * cdf, cdf + val * (0.5 * (1.0 - th * th) * (ROOT * (1.0 + 3.0 * CUBIC * (val * val))))


def gelu_only(val):
    return val * (0.5 * (1.0 + jnp.tanh(ROOT * (val + CUBIC * (val * val * val)))))


def dot_nn(a, b):
    return jnp.dot(a, b, preferred_element_type=F32)


def pipe_kernel(norm, x_hbm, t_hbm, w1_hbm, w2_hbm,
                h_out, g_out, a_out, e_out, loss_out,
                w1, w2, w1t, w2t, xs, us, acts, tgt, act_now, part, recv, outb, loss_acc, loss_src, loss_dst,
                w_sem, in_sem, x_sem, part_sem, recv_sem, leaf_sem, peer_sem, copy_sem, loss_sem, loss_got):
    n_stage, n_tp = 4, 4
    _, n, unit, width = xs.shape
    hid = us.shape[3]
    cw = width // N_CHUNK
    stage = lax.axis_index('pp')
    z = lax.axis_index('tp')
    last = n_stage - 1
    is_center = (z == 1) | (z == 2)
    is_leaf = (z == 0) | (z == 3)
    center_i = is_center.astype(jnp.int32)
    partner = z + 1 - 2 * (z % 2)
    peer = partner + center_i * (3 - z - partner)
    at_last_i = (stage == last).astype(jnp.int32)
    gap = GAP * (1 - at_last_i)

    w_copies = []
    for k in range(2):
        w_copies.append((pltpu.make_async_copy(w1_hbm.at[k], w1.at[k], w_sem.at[0, k]),
                         pltpu.make_async_copy(w2_hbm.at[k], w2.at[k], w_sem.at[1, k])))
    x_copy = pltpu.make_async_copy(x_hbm, xs.at[0], in_sem.at[0])
    t_copy = pltpu.make_async_copy(t_hbm, tgt, in_sem.at[1])

    @pl.when(stage == 0)
    def _():
        x_copy.start()

    for pair in w_copies:
        for copy in pair:
            copy.start()
    t_copy.start()
    loss_acc[...] = jnp.zeros_like(loss_acc)

    barrier = pltpu.get_barrier_semaphore()
    for ds in range(n_stage):
        for dz in range(n_tp):
            if ds or dz:
                pl.semaphore_signal(barrier, inc=1, device_id={'pp': (stage + ds) % n_stage, 'tp': (z + dz) % n_tp}, device_id_type=MESH)
    pl.semaphore_wait(barrier, n_stage * n_tp - 1)

    @pl.when(stage == 0)
    def _():
        x_copy.wait()

    @pl.when(stage == last)
    def _():
        t_copy.wait()

    def flip():
        for src, dst in ((w1, w1t), (w2, w2t)):
            _, rows, columns = src.shape

            def tile_row(i, carry):
                k = i // (rows // TILE)
                at_row = pl.ds(pl.multiple_of((i % (rows // TILE)) * TILE, TILE), TILE)
                for j in range(columns // TILE):
                    js = pl.ds(j * TILE, TILE)
                    dst[k, js, at_row] = src[k, at_row, js].T
                return carry

            lax.fori_loop(0, 2 * (rows // TILE), tile_row, 0)

    @pl.when(stage > 0)
    def _():
        for pair in w_copies:
            for copy in pair:
                copy.wait()
        flip()

    def cols(c):
        return pl.ds(c * cw, cw)

    def part_send(p, slot, c):
        return pltpu.make_async_remote_copy(
            src_ref=part.at[p, slot, c], dst_ref=recv.at[center_i, p, slot, c],
            send_sem=part_sem.at[p, slot, c], recv_sem=recv_sem.at[center_i, p, slot, c],
            device_id={'pp': stage, 'tp': peer}, device_id_type=MESH)

    def part_arrival(kind, p, slot, c):
        return pltpu.make_async_remote_copy(
            src_ref=part.at[p, slot, c], dst_ref=recv.at[kind, p, slot, c],
            send_sem=part_sem.at[p, slot, c], recv_sem=recv_sem.at[kind, p, slot, c],
            device_id={'pp': stage, 'tp': peer}, device_id_type=MESH)

    def out_send(p, slot, c, q, m, to_stage, to_tp, sem):
        return pltpu.make_async_remote_copy(
            src_ref=outb.at[p, slot, c], dst_ref=xs.at[q, m, :, cols(c)],
            send_sem=sem.at[p, slot, c], recv_sem=x_sem.at[q, m, c],
            device_id={'pp': to_stage, 'tp': to_tp}, device_id_type=MESH)

    def at(v):
        fwd = (v >= 0) & (v < n)
        bwd = (v >= n + gap) & (v < 2 * n + gap)
        bwd_i = (v >= n).astype(jnp.int32)
        m = v - bwd_i * (n + gap)
        return fwd, bwd, bwd_i, m, m + bwd_i * n

    def arrived(q, m):
        for c in range(N_CHUNK):
            out_send(0, 0, c, q, m, stage, z, leaf_sem).wait_recv()

    def free_part(p, i):
        @pl.when(i >= SLOTS)
        def _():
            for c in range(N_CHUNK):
                part_send(p, i % SLOTS, c).wait_send()

    def send_part(p, slot, c):
        @pl.when(is_leaf)
        def _():
            part_send(p, slot, c).start()

    def compute(v, p):
        fwd, bwd, _, m, i = at(v)
        slot = i % SLOTS

        @pl.when(fwd)
        def _():
            @pl.when((m == 0) & (stage == 0))
            def _():
                w_copies[p][0].wait()
            if p == 0:
                @pl.when(stage > 0)
                def _():
                    arrived(0, m)
            else:
                @pl.when(is_leaf)
                def _():
                    arrived(1, m)
            free_part(p, i)
            for j in range(hid // BLOCK):
                js = pl.ds(j * BLOCK, BLOCK)
                pre = dot_nn(xs[p, m], w1[p, :, js]).astype(BF16)
                us[p, m, :, js] = pre
                act_now[:, js] = gelu_only(pre.astype(F32)).astype(BF16)

            @pl.when((m == 0) & (stage == 0))
            def _():
                w_copies[p][1].wait()
            for c in range(N_CHUNK):
                part[p, slot, c] = dot_nn(act_now[...], w2[p, :, cols(c)])
                send_part(p, slot, c)

        @pl.when(bwd)
        def _():
            k = 1 - p
            if p == 0:
                @pl.when(is_leaf | (stage < last))
                def _():
                    arrived(2, m)
            else:
                @pl.when(is_leaf)
                def _():
                    arrived(3, m)

            def outs():
                return (pltpu.make_async_copy(xs.at[k, m], h_out.at[k, m], copy_sem.at[p, 0]),
                        pltpu.make_async_copy(xs.at[2 + p, m], g_out.at[k, m], copy_sem.at[p, 1]),
                        pltpu.make_async_copy(acts.at[k, m], a_out.at[k, m], copy_sem.at[p, 2]),
                        pltpu.make_async_copy(us.at[k, m], e_out.at[k, m], copy_sem.at[p, 3]))

            @pl.when(m > 0)
            def _():
                for copy in outs():
                    copy.wait()
            for j in range(hid // BLOCK):
                js = pl.ds(j * BLOCK, BLOCK)
                grad = dot_nn(xs[2 + p, m], w2t[k, :, js])
                act, slope = gelu_parts(us[k, m, :, js].astype(F32))
                acts[k, m, :, js] = act.astype(BF16)
                err = (slope * grad).astype(BF16)
                us[k, m, :, js] = err
                act_now[:, js] = err

            def down():
                free_part(p, i)
                for c in range(N_CHUNK):
                    part[p, slot, c] = dot_nn(act_now[...], w1t[k, :, cols(c)])
                    send_part(p, slot, c)

            if p == 0:
                down()
            else:
                pl.when(stage > 0)(down)
            for copy in outs():
                copy.start()

    def sums(v, p):
        fwd, bwd, bwd_i, m, i = at(v)
        live = fwd | bwd if p == 0 else fwd | (bwd & (stage > 0))
        return live & is_center, fwd, bwd_i, m, i, i % SLOTS

    def add_leaf(v, p, chunks):
        live, _, _, _, _, slot = sums(v, p)

        @pl.when(live)
        def _():
            for c in chunks:
                part_arrival(0, p, slot, c).wait_recv()
                part[p, slot, c] = part[p, slot, c] + recv[0, p, slot, c]
                part_send(p, slot, c).start()

    def finish(v, p, chunks):
        live, fwd, bwd_i, m, i, slot = sums(v, p)
        if p == 0:
            to_stage, q = stage, 1 + 2 * bwd_i
        else:
            home = (1 - bwd_i) * at_last_i
            to_stage, q = stage + (1 - home) * (1 - 2 * bwd_i), 2 * bwd_i + 2 * home

        @pl.when(live)
        def _():
            @pl.when(i >= SLOTS)
            def _():
                for c in chunks:
                    out_send(p, slot, c, q, m, to_stage, partner, leaf_sem).wait_send()
            if p == 1:
                @pl.when((i >= SLOTS) & ((stage < last) | (i >= SLOTS + n)))
                def _():
                    for c in chunks:
                        out_send(p, slot, c, q, m, to_stage, z, peer_sem).wait_send()
            for c in chunks:
                part_arrival(1, p, slot, c).wait_recv()
                res = (xs[2 * bwd_i + p, m, :, cols(c)].astype(F32) + (part[p, slot, c] + recv[1, p, slot, c])).astype(BF16)
                if p == 0:
                    outb[p, slot, c] = res
                    xs[q, m, :, cols(c)] = res
                else:
                    @pl.when((stage < last) | (bwd_i == 1))
                    def _():
                        outb[p, slot, c] = res
                        out_send(p, slot, c, q, m, to_stage, z, peer_sem).start()

                    @pl.when((stage == last) & (bwd_i == 0))
                    def _():
                        diff = res.astype(F32) - tgt[m, :, cols(c)].astype(F32)
                        grad = (diff * norm).astype(BF16)
                        outb[p, slot, c] = grad
                        xs[q, m, :, cols(c)] = grad
                        sq = diff * diff
                        acc = loss_acc[...]
                        for r in range(unit // 8):
                            for b in range(cw // 128):
                                acc = acc + sq[r * 8:(r + 1) * 8, b * 128:(b + 1) * 128]
                        loss_acc[...] = acc
                out_send(p, slot, c, q, m, to_stage, partner, leaf_sem).start()

    def step(t, carry):
        @pl.when((stage == 0) & (t == n + GAP - 1))
        def _():
            flip()

        for kind, lag, p, chunks in ORDER:
            if kind == 'dot':
                compute(t - lag - p * (OUTER_LAG - lag) * (1 - center_i), p)
            elif kind == 'sum':
                add_leaf(t - lag, p, chunks)
            else:
                finish(t - lag, p, chunks)
        return carry

    lax.fori_loop(0, 2 * n + GAP + 3, step, 0)

    @pl.when(stage < last)
    def _():
        t_copy.wait()

    for p in range(2):
        for slot in range(SLOTS):
            for c in range(N_CHUNK):
                part_send(p, slot, c).wait_send()

                @pl.when(is_center)
                def _():
                    out_send(p, slot, c, 0, 0, stage, partner, leaf_sem).wait_send()
                    if p == 1:
                        out_send(p, slot, c, 0, 0, stage, z, peer_sem).wait_send()
        k = 1 - p
        pltpu.make_async_copy(xs.at[k, 0], h_out.at[k, 0], copy_sem.at[p, 0]).wait()
        pltpu.make_async_copy(xs.at[2 + p, 0], g_out.at[k, 0], copy_sem.at[p, 1]).wait()
        pltpu.make_async_copy(acts.at[k, 0], a_out.at[k, 0], copy_sem.at[p, 2]).wait()
        pltpu.make_async_copy(us.at[k, 0], e_out.at[k, 0], copy_sem.at[p, 3]).wait()

    def loss_send(idx, to_stage, to_tp):
        return pltpu.make_async_remote_copy(
            src_ref=loss_src, dst_ref=loss_dst, send_sem=loss_sem.at[idx], recv_sem=loss_got.at[0],
            device_id={'pp': to_stage, 'tp': to_tp}, device_id_type=MESH)

    sender = is_center & (stage == last)

    @pl.when(sender)
    def _():
        total = jnp.sum(loss_acc[...]) * 0.5 * norm
        value = jnp.full(loss_src.shape, total, F32)
        loss_src[...] = value
        loss_out[...] = value
        sends = [loss_send(2 * s + b, s, z if b else partner) for s in range(n_stage) for b in range(2) if not (s == last and b)]
        for send in sends:
            send.start()
        for send in sends:
            send.wait_send()

    @pl.when(is_leaf | (stage < last))
    def _():
        loss_send(0, stage, z).wait_recv()
        loss_out[...] = loss_dst[...]


def solution(mesh):
    def stage_body(x_micro, targets, w_in, w_out):
        n_micro, n_token, width = x_micro.shape
        hid = w_in.shape[3]
        n = n_micro * n_token // UNIT
        norm = 1.0 / (n_micro * n_token * width)
        cw = width // N_CHUNK
        any_spec = pl.BlockSpec(memory_space=pl.ANY)
        h, g, a, e, loss = pl.pallas_call(
            functools.partial(pipe_kernel, norm),
            out_shape=(
                jax.ShapeDtypeStruct((2, n, UNIT, width), BF16),
                jax.ShapeDtypeStruct((2, n, UNIT, width), BF16),
                jax.ShapeDtypeStruct((2, n, UNIT, hid), BF16),
                jax.ShapeDtypeStruct((2, n, UNIT, hid), BF16),
                jax.ShapeDtypeStruct((8, 128), F32),
            ),
            in_specs=[any_spec] * 4,
            out_specs=(any_spec, any_spec, any_spec, any_spec, pl.BlockSpec(memory_space=pltpu.VMEM)),
            scratch_shapes=[
                pltpu.VMEM((2, width, hid), BF16),
                pltpu.VMEM((2, hid, width), BF16),
                pltpu.VMEM((2, hid, width), BF16),
                pltpu.VMEM((2, width, hid), BF16),
                pltpu.VMEM((4, n, UNIT, width), BF16),
                pltpu.VMEM((2, n, UNIT, hid), BF16),
                pltpu.VMEM((2, n, UNIT, hid), BF16),
                pltpu.VMEM((n, UNIT, width), BF16),
                pltpu.VMEM((UNIT, hid), BF16),
                pltpu.VMEM((2, SLOTS, N_CHUNK, UNIT, cw), F32),
                pltpu.VMEM((2, 2, SLOTS, N_CHUNK, UNIT, cw), F32),
                pltpu.VMEM((2, SLOTS, N_CHUNK, UNIT, cw), BF16),
                pltpu.VMEM((8, 128), F32),
                pltpu.VMEM((8, 128), F32),
                pltpu.VMEM((8, 128), F32),
                pltpu.SemaphoreType.DMA((2, 2)),
                pltpu.SemaphoreType.DMA((2,)),
                pltpu.SemaphoreType.DMA((4, n, N_CHUNK)),
                pltpu.SemaphoreType.DMA((2, SLOTS, N_CHUNK)),
                pltpu.SemaphoreType.DMA((2, 2, SLOTS, N_CHUNK)),
                pltpu.SemaphoreType.DMA((2, SLOTS, N_CHUNK)),
                pltpu.SemaphoreType.DMA((2, SLOTS, N_CHUNK)),
                pltpu.SemaphoreType.DMA((2, 4)),
                pltpu.SemaphoreType.DMA((8,)),
                pltpu.SemaphoreType.DMA((1,)),
            ],
            compiler_params=pltpu.CompilerParams(collective_id=0, has_side_effects=True, vmem_limit_bytes=67043328),
        )(x_micro.reshape(n, UNIT, width), targets.reshape(n, UNIT, width), w_in[0], w_out[0])

        h, g = (v.reshape(2, n * UNIT, width) for v in (h, g))
        a, e = (v.reshape(2, n * UNIT, hid) for v in (a, e))
        grad_first = jnp.einsum('kbd,kbf->kdf', h, e, preferred_element_type=F32)
        grad_second = jnp.einsum('kbf,kbd->kfd', a, g, preferred_element_type=F32)
        return grad_first[None], grad_second[None], loss[0, :1]

    data_spec = P('dp', None, None)
    return jax.shard_map(stage_body, mesh=mesh, in_specs=(data_spec, data_spec, P('pp', None, None, 'tp'), P('pp', None, 'tp', None)), out_specs=(P(('dp', 'pp'), None, None, 'tp'), P(('dp', 'pp'), None, 'tp', None), P('dp')), check_vma=False)
```

```python
import functools
import math

import jax
import jax.numpy as jnp
from jax import lax
from jax.experimental import pallas as pl
from jax.experimental.pallas import tpu as pltpu
from jax.sharding import PartitionSpec as P

UNIT = 32
N_CHUNK = 3
SLOTS = 4
BLOCK = 512
GRAD_BLOCKS = 3
TILE = 256
GAP = 4

MESH = pl.DeviceIdType.MESH
F32 = jnp.float32
BF16 = jnp.bfloat16
ROOT = math.sqrt(2 / math.pi)
CUBIC = 0.044715


ALL = tuple(range(N_CHUNK))
ORDER = (('sum', 3, 1, (1,)), ('dot', 0, 0, ALL), ('sum', 3, 1, (2,)), ('end', 1, 0, (1, 0)), ('sum', 0, 0, (0, 1)), ('end', 1, 0, (2,)),
         ('dot', 1, 1, ALL), ('end', 3, 1, (0,)), ('sum', 0, 0, (2,)), ('end', 3, 1, (1,)), ('sum', 2, 1, (0,)), ('end', 3, 1, (2,)))
OUTER_LAG = 2


def gelu_parts(val):
    th = jnp.tanh(ROOT * (val + CUBIC * (val * val * val)))
    cdf = 0.5 * (1.0 + th)
    return val * cdf, cdf + val * (0.5 * (1.0 - th * th) * (ROOT * (1.0 + 3.0 * CUBIC * (val * val))))


def gelu_only(val):
    return val * (0.5 * (1.0 + jnp.tanh(ROOT * (val + CUBIC * (val * val * val)))))


def dot_nn(a, b):
    return jnp.dot(a, b, preferred_element_type=F32)


def pipe_kernel(norm, x_hbm, t_hbm, w1_hbm, w2_hbm,
                h_out, g_out, a_out, e_out, loss_out,
                w1, w2, w1t, w2t, xs, us, acts, tgt, act_now, part, recv, outb, loss_acc, loss_src, loss_dst,
                w_sem, in_sem, x_sem, part_sem, recv_sem, leaf_sem, peer_sem, copy_sem, loss_sem, loss_got):
    n_stage, n_tp = 4, 4
    _, n, unit, width = xs.shape
    hid = us.shape[3]
    cw = width // N_CHUNK
    stage = lax.axis_index('pp')
    z = lax.axis_index('tp')
    last = n_stage - 1
    is_center = (z == 1) | (z == 2)
    is_leaf = (z == 0) | (z == 3)
    center_i = is_center.astype(jnp.int32)
    partner = z + 1 - 2 * (z % 2)
    peer = partner + center_i * (3 - z - partner)
    at_last_i = (stage == last).astype(jnp.int32)
    gap = GAP * (1 - at_last_i)

    w_copies = []
    for k in range(2):
        w_copies.append((pltpu.make_async_copy(w1_hbm.at[k], w1.at[k], w_sem.at[0, k]),
                         pltpu.make_async_copy(w2_hbm.at[k], w2.at[k], w_sem.at[1, k])))
    x_copy = pltpu.make_async_copy(x_hbm, xs.at[0], in_sem.at[0])
    t_copy = pltpu.make_async_copy(t_hbm, tgt, in_sem.at[1])

    @pl.when(stage == 0)
    def _():
        x_copy.start()

    for copy in w_copies[0]:
        copy.start()
    loss_acc[...] = jnp.zeros_like(loss_acc)

    barrier = pltpu.get_barrier_semaphore()
    for ds in range(n_stage):
        for dz in range(n_tp):
            if ds or dz:
                pl.semaphore_signal(barrier, inc=1, device_id={'pp': (stage + ds) % n_stage, 'tp': (z + dz) % n_tp}, device_id_type=MESH)
    pl.semaphore_wait(barrier, n_stage * n_tp - 1)

    for copy in w_copies[1]:
        copy.start()
    t_copy.start()

    @pl.when(stage == 0)
    def _():
        x_copy.wait()

    @pl.when(stage == last)
    def _():
        t_copy.wait()

    def flip():
        for src, dst in ((w1, w1t), (w2, w2t)):
            _, rows, columns = src.shape

            def tile_row(i, carry):
                k = i // (rows // TILE)
                at_row = pl.ds(pl.multiple_of((i % (rows // TILE)) * TILE, TILE), TILE)
                for j in range(columns // TILE):
                    js = pl.ds(j * TILE, TILE)
                    dst[k, js, at_row] = src[k, at_row, js].T
                return carry

            lax.fori_loop(0, 2 * (rows // TILE), tile_row, 0)

    @pl.when(stage > 0)
    def _():
        for pair in w_copies:
            for copy in pair:
                copy.wait()
        flip()

    def cols(c):
        return pl.ds(c * cw, cw)

    def part_send(p, slot, c):
        return pltpu.make_async_remote_copy(
            src_ref=part.at[p, slot, c], dst_ref=recv.at[center_i, p, slot, c],
            send_sem=part_sem.at[p, slot, c], recv_sem=recv_sem.at[center_i, p, slot, c],
            device_id={'pp': stage, 'tp': peer}, device_id_type=MESH)

    def part_arrival(kind, p, slot, c):
        return pltpu.make_async_remote_copy(
            src_ref=part.at[p, slot, c], dst_ref=recv.at[kind, p, slot, c],
            send_sem=part_sem.at[p, slot, c], recv_sem=recv_sem.at[kind, p, slot, c],
            device_id={'pp': stage, 'tp': peer}, device_id_type=MESH)

    def out_send(p, slot, c, q, m, to_stage, to_tp, sem):
        return pltpu.make_async_remote_copy(
            src_ref=outb.at[p, slot, c], dst_ref=xs.at[q, m, :, cols(c)],
            send_sem=sem.at[p, slot, c], recv_sem=x_sem.at[q, m, c],
            device_id={'pp': to_stage, 'tp': to_tp}, device_id_type=MESH)

    def at(v):
        fwd = (v >= 0) & (v < n)
        bwd = (v >= n + gap) & (v < 2 * n + gap)
        bwd_i = (v >= n).astype(jnp.int32)
        m = v - bwd_i * (n + gap)
        return fwd, bwd, bwd_i, m, m + bwd_i * n

    def arrived(q, m):
        for c in range(N_CHUNK):
            out_send(0, 0, c, q, m, stage, z, leaf_sem).wait_recv()

    def free_part(p, i):
        @pl.when(i >= SLOTS)
        def _():
            for c in range(N_CHUNK):
                part_send(p, i % SLOTS, c).wait_send()

    def send_part(p, slot, c):
        @pl.when(is_leaf)
        def _():
            part_send(p, slot, c).start()

    def compute(v, p):
        fwd, bwd, _, m, i = at(v)
        slot = i % SLOTS

        @pl.when(fwd)
        def _():
            @pl.when((m == 0) & (stage == 0))
            def _():
                w_copies[p][0].wait()
            if p == 0:
                @pl.when(stage > 0)
                def _():
                    arrived(0, m)
            else:
                @pl.when(is_leaf)
                def _():
                    arrived(1, m)
            free_part(p, i)
            for j in range(hid // BLOCK):
                js = pl.ds(j * BLOCK, BLOCK)
                pre = dot_nn(xs[p, m], w1[p, :, js]).astype(BF16)
                us[p, m, :, js] = pre
                act_now[:, js] = gelu_only(pre.astype(F32)).astype(BF16)

            @pl.when((m == 0) & (stage == 0))
            def _():
                w_copies[p][1].wait()
            for c in range(N_CHUNK):
                part[p, slot, c] = dot_nn(act_now[...], w2[p, :, cols(c)])
                send_part(p, slot, c)

        @pl.when(bwd)
        def _():
            k = 1 - p
            if p == 0:
                @pl.when(is_leaf | (stage < last))
                def _():
                    arrived(2, m)
            else:
                @pl.when(is_leaf)
                def _():
                    arrived(3, m)

            def outs():
                return (pltpu.make_async_copy(xs.at[k, m], h_out.at[k, m], copy_sem.at[p, 0]),
                        pltpu.make_async_copy(xs.at[2 + p, m], g_out.at[k, m], copy_sem.at[p, 1]),
                        pltpu.make_async_copy(acts.at[k, m], a_out.at[k, m], copy_sem.at[p, 2]),
                        pltpu.make_async_copy(us.at[k, m], e_out.at[k, m], copy_sem.at[p, 3]))

            @pl.when(m > 0)
            def _():
                for copy in outs():
                    copy.wait()
            for j in range(hid // BLOCK):
                js = pl.ds(j * BLOCK, BLOCK)
                grad = dot_nn(xs[2 + p, m], w2t[k, :, js])
                act, slope = gelu_parts(us[k, m, :, js].astype(F32))
                acts[k, m, :, js] = act.astype(BF16)
                err = (slope * grad).astype(BF16)
                us[k, m, :, js] = err
                act_now[:, js] = err

            def down():
                free_part(p, i)
                for c in range(N_CHUNK):
                    part[p, slot, c] = dot_nn(act_now[...], w1t[k, :, cols(c)])
                    send_part(p, slot, c)

            if p == 0:
                down()
            else:
                pl.when(stage > 0)(down)
            for copy in outs():
                copy.start()

    def sums(v, p):
        fwd, bwd, bwd_i, m, i = at(v)
        live = fwd | bwd if p == 0 else fwd | (bwd & (stage > 0))
        return live & is_center, fwd, bwd_i, m, i, i % SLOTS

    def add_leaf(v, p, chunks):
        live, _, _, _, _, slot = sums(v, p)

        @pl.when(live)
        def _():
            for c in chunks:
                part_arrival(0, p, slot, c).wait_recv()
                part[p, slot, c] = part[p, slot, c] + recv[0, p, slot, c]
                part_send(p, slot, c).start()

    def finish(v, p, chunks):
        live, fwd, bwd_i, m, i, slot = sums(v, p)
        if p == 0:
            to_stage, q = stage, 1 + 2 * bwd_i
        else:
            home = (1 - bwd_i) * at_last_i
            to_stage, q = stage + (1 - home) * (1 - 2 * bwd_i), 2 * bwd_i + 2 * home

        @pl.when(live)
        def _():
            @pl.when(i >= SLOTS)
            def _():
                for c in chunks:
                    out_send(p, slot, c, q, m, to_stage, partner, leaf_sem).wait_send()
            if p == 1:
                @pl.when((i >= SLOTS) & ((stage < last) | (i >= SLOTS + n)))
                def _():
                    for c in chunks:
                        out_send(p, slot, c, q, m, to_stage, z, peer_sem).wait_send()
            for c in chunks:
                part_arrival(1, p, slot, c).wait_recv()
                res = (xs[2 * bwd_i + p, m, :, cols(c)].astype(F32) + (part[p, slot, c] + recv[1, p, slot, c])).astype(BF16)
                if p == 0:
                    outb[p, slot, c] = res
                    xs[q, m, :, cols(c)] = res
                else:
                    @pl.when((stage < last) | (bwd_i == 1))
                    def _():
                        outb[p, slot, c] = res
                        out_send(p, slot, c, q, m, to_stage, z, peer_sem).start()

                    @pl.when((stage == last) & (bwd_i == 0))
                    def _():
                        diff = res.astype(F32) - tgt[m, :, cols(c)].astype(F32)
                        grad = (diff * norm).astype(BF16)
                        outb[p, slot, c] = grad
                        xs[q, m, :, cols(c)] = grad
                        sq = diff * diff
                        acc = loss_acc[...]
                        for r in range(unit // 8):
                            for b in range(cw // 128):
                                acc = acc + sq[r * 8:(r + 1) * 8, b * 128:(b + 1) * 128]
                        loss_acc[...] = acc
                out_send(p, slot, c, q, m, to_stage, partner, leaf_sem).start()

    def step(t, carry):
        @pl.when((stage == 0) & (t == n + GAP - 1))
        def _():
            flip()

        for kind, lag, p, chunks in ORDER:
            if kind == 'dot':
                compute(t - lag - p * (OUTER_LAG - lag) * (1 - center_i), p)
            elif kind == 'sum':
                add_leaf(t - lag, p, chunks)
            else:
                finish(t - lag, p, chunks)
        return carry

    lax.fori_loop(0, 2 * n + GAP + 3, step, 0)

    @pl.when(stage < last)
    def _():
        t_copy.wait()

    for p in range(2):
        for slot in range(SLOTS):
            for c in range(N_CHUNK):
                part_send(p, slot, c).wait_send()

                @pl.when(is_center)
                def _():
                    out_send(p, slot, c, 0, 0, stage, partner, leaf_sem).wait_send()
                    if p == 1:
                        out_send(p, slot, c, 0, 0, stage, z, peer_sem).wait_send()
        k = 1 - p
        pltpu.make_async_copy(xs.at[k, 0], h_out.at[k, 0], copy_sem.at[p, 0]).wait()
        pltpu.make_async_copy(xs.at[2 + p, 0], g_out.at[k, 0], copy_sem.at[p, 1]).wait()
        pltpu.make_async_copy(acts.at[k, 0], a_out.at[k, 0], copy_sem.at[p, 2]).wait()
        pltpu.make_async_copy(us.at[k, 0], e_out.at[k, 0], copy_sem.at[p, 3]).wait()

    def loss_send(idx, to_stage, to_tp):
        return pltpu.make_async_remote_copy(
            src_ref=loss_src, dst_ref=loss_dst, send_sem=loss_sem.at[idx], recv_sem=loss_got.at[0],
            device_id={'pp': to_stage, 'tp': to_tp}, device_id_type=MESH)

    sender = is_center & (stage == last)

    @pl.when(sender)
    def _():
        total = jnp.sum(loss_acc[...]) * 0.5 * norm
        value = jnp.full(loss_src.shape, total, F32)
        loss_src[...] = value
        loss_out[...] = value
        sends = [loss_send(2 * s + b, s, z if b else partner) for s in range(n_stage) for b in range(2) if not (s == last and b)]
        for send in sends:
            send.start()
        for send in sends:
            send.wait_send()

    @pl.when(is_leaf | (stage < last))
    def _():
        loss_send(0, stage, z).wait_recv()
        loss_out[...] = loss_dst[...]


def weight_grads(h_ref, e_ref, a_ref, g_ref, loss_ref, first_ref, second_ref, total_ref):
    half = pl.program_id(0)

    def over_tokens(left, right):
        return lax.dot_general(left, right, (((0,), (0,)), ((), ())), preferred_element_type=F32)

    @pl.when(half == 0)
    def _():
        total_ref[0] = jnp.max(loss_ref[...])
        first_ref[0] = over_tokens(h_ref[0], e_ref[0])

    @pl.when(half == 1)
    def _():
        second_ref[0] = over_tokens(a_ref[0], g_ref[0])


def solution(mesh):
    def stage_body(x_micro, targets, w_in, w_out):
        n_micro, n_token, width = x_micro.shape
        hid = w_in.shape[3]
        n = n_micro * n_token // UNIT
        norm = 1.0 / (n_micro * n_token * width)
        cw = width // N_CHUNK
        any_spec = pl.BlockSpec(memory_space=pl.ANY)
        h, g, a, e, loss = pl.pallas_call(
            functools.partial(pipe_kernel, norm),
            out_shape=(
                jax.ShapeDtypeStruct((2, n, UNIT, width), BF16),
                jax.ShapeDtypeStruct((2, n, UNIT, width), BF16),
                jax.ShapeDtypeStruct((2, n, UNIT, hid), BF16),
                jax.ShapeDtypeStruct((2, n, UNIT, hid), BF16),
                jax.ShapeDtypeStruct((8, 128), F32),
            ),
            in_specs=[any_spec] * 4,
            out_specs=(any_spec, any_spec, any_spec, any_spec, pl.BlockSpec(memory_space=pltpu.VMEM)),
            scratch_shapes=[
                pltpu.VMEM((2, width, hid), BF16),
                pltpu.VMEM((2, hid, width), BF16),
                pltpu.VMEM((2, hid, width), BF16),
                pltpu.VMEM((2, width, hid), BF16),
                pltpu.VMEM((4, n, UNIT, width), BF16),
                pltpu.VMEM((2, n, UNIT, hid), BF16),
                pltpu.VMEM((2, n, UNIT, hid), BF16),
                pltpu.VMEM((n, UNIT, width), BF16),
                pltpu.VMEM((UNIT, hid), BF16),
                pltpu.VMEM((2, SLOTS, N_CHUNK, UNIT, cw), F32),
                pltpu.VMEM((2, 2, SLOTS, N_CHUNK, UNIT, cw), F32),
                pltpu.VMEM((2, SLOTS, N_CHUNK, UNIT, cw), BF16),
                pltpu.VMEM((8, 128), F32),
                pltpu.VMEM((8, 128), F32),
                pltpu.VMEM((8, 128), F32),
                pltpu.SemaphoreType.DMA((2, 2)),
                pltpu.SemaphoreType.DMA((2,)),
                pltpu.SemaphoreType.DMA((4, n, N_CHUNK)),
                pltpu.SemaphoreType.DMA((2, SLOTS, N_CHUNK)),
                pltpu.SemaphoreType.DMA((2, 2, SLOTS, N_CHUNK)),
                pltpu.SemaphoreType.DMA((2, SLOTS, N_CHUNK)),
                pltpu.SemaphoreType.DMA((2, SLOTS, N_CHUNK)),
                pltpu.SemaphoreType.DMA((2, 4)),
                pltpu.SemaphoreType.DMA((8,)),
                pltpu.SemaphoreType.DMA((1,)),
            ],
            compiler_params=pltpu.CompilerParams(collective_id=0, has_side_effects=True, vmem_limit_bytes=67043328),
        )(x_micro.reshape(n, UNIT, width), targets.reshape(n, UNIT, width), w_in[0], w_out[0])

        h, g = (v.reshape(2, n * UNIT, width) for v in (h, g))
        a, e = (v.reshape(2, n * UNIT, hid) for v in (a, e))
        tokens = n * UNIT
        grad_first, grad_second, total = pl.pallas_call(
            weight_grads,
            grid=(2, 2, GRAD_BLOCKS),
            out_shape=(
                jax.ShapeDtypeStruct((2, width, hid), F32),
                jax.ShapeDtypeStruct((2, hid, width), F32),
                jax.ShapeDtypeStruct((1,), F32),
            ),
            in_specs=[
                pl.BlockSpec((1, tokens, width), lambda i, k, j: (k + i * (1 - k), 0, 0)),
                pl.BlockSpec((1, tokens, hid // GRAD_BLOCKS), lambda i, k, j: (k + i * (1 - k), 0, j + i * (GRAD_BLOCKS - 1 - j))),
                pl.BlockSpec((1, tokens, hid), lambda i, k, j: (k * i, 0, 0)),
                pl.BlockSpec((1, tokens, width // GRAD_BLOCKS), lambda i, k, j: (k * i, 0, j * i)),
                pl.BlockSpec(memory_space=pltpu.VMEM),
            ],
            out_specs=(
                pl.BlockSpec((1, width, hid // GRAD_BLOCKS), lambda i, k, j: (k + i * (1 - k), 0, j + i * (GRAD_BLOCKS - 1 - j))),
                pl.BlockSpec((1, hid, width // GRAD_BLOCKS), lambda i, k, j: (k * i, 0, j * i)),
                pl.BlockSpec(memory_space=pltpu.SMEM),
            ),
            compiler_params=pltpu.CompilerParams(vmem_limit_bytes=56 * 1024 * 1024),
        )(h, e, a, g, loss)
        return grad_first[None], grad_second[None], total

    data_spec = P('dp', None, None)
    return jax.shard_map(stage_body, mesh=mesh, in_specs=(data_spec, data_spec, P('pp', None, None, 'tp'), P('pp', None, 'tp', None)), out_specs=(P(('dp', 'pp'), None, None, 'tp'), P(('dp', 'pp'), None, 'tp', None), P('dp')), check_vma=False)
```

```python
import functools
import math

import jax
import jax.numpy as jnp
from jax import lax
from jax.experimental import pallas as pl
from jax.experimental.pallas import tpu as pltpu
from jax.sharding import PartitionSpec as P

UNIT = 32
N_CHUNK = 3
SLOTS = 4
BLOCK = 512
GRAD_BLOCKS = 3
TILE = 256
GAP = 4

MESH = pl.DeviceIdType.MESH
F32 = jnp.float32
BF16 = jnp.bfloat16
ROOT = math.sqrt(2 / math.pi)
CUBIC = 0.044715


ALL = tuple(range(N_CHUNK))
ORDER = (('sum', 3, 1, (1,)), ('dot', 0, 0, ALL), ('sum', 3, 1, (2,)), ('end', 1, 0, (1, 0)), ('sum', 0, 0, (0, 1)), ('end', 1, 0, (2,)),
         ('dot', 1, 1, ALL), ('end', 3, 1, (0,)), ('sum', 0, 0, (2,)), ('end', 3, 1, (1,)), ('sum', 2, 1, (0,)), ('end', 3, 1, (2,)))
OUTER_LAG = 2


def gelu_parts(val):
    th = jnp.tanh(ROOT * (val + CUBIC * (val * val * val)))
    cdf = 0.5 * (1.0 + th)
    return val * cdf, cdf + val * (0.5 * (1.0 - th * th) * (ROOT * (1.0 + 3.0 * CUBIC * (val * val))))


def gelu_only(val):
    return val * (0.5 * (1.0 + jnp.tanh(ROOT * (val + CUBIC * (val * val * val)))))


def dot_nn(a, b):
    return jnp.dot(a, b, preferred_element_type=F32)


def pipe_kernel(norm, x_hbm, t_hbm, w1_hbm, w2_hbm,
                h_out, g_out, a_out, e_out, loss_out,
                w1, w2, w1t, w2t, xs, us, acts, tgt, act_now, part, recv, outb, loss_acc, loss_src, loss_dst,
                w_sem, in_sem, x_sem, part_sem, recv_sem, leaf_sem, peer_sem, copy_sem, loss_sem, loss_got):
    n_stage, n_tp = 4, 4
    _, n, unit, width = xs.shape
    hid = us.shape[3]
    cw = width // N_CHUNK
    stage = lax.axis_index('pp')
    z = lax.axis_index('tp')
    last = n_stage - 1
    is_center = (z == 1) | (z == 2)
    is_leaf = (z == 0) | (z == 3)
    center_i = is_center.astype(jnp.int32)
    partner = z + 1 - 2 * (z % 2)
    peer = partner + center_i * (3 - z - partner)
    at_last_i = (stage == last).astype(jnp.int32)
    gap = GAP * (1 - at_last_i)

    w_copies = []
    for k in range(2):
        w_copies.append((pltpu.make_async_copy(w1_hbm.at[k], w1.at[k], w_sem.at[0, k]),
                         pltpu.make_async_copy(w2_hbm.at[k], w2.at[k], w_sem.at[1, k])))
    x_copy = pltpu.make_async_copy(x_hbm, xs.at[0], in_sem.at[0])
    t_copy = pltpu.make_async_copy(t_hbm, tgt, in_sem.at[1])

    @pl.when(stage == 0)
    def _():
        x_copy.start()

    for copy in w_copies[0]:
        copy.start()
    loss_acc[...] = jnp.zeros_like(loss_acc)

    barrier = pltpu.get_barrier_semaphore()
    for ds in range(n_stage):
        for dz in range(n_tp):
            if ds or dz:
                pl.semaphore_signal(barrier, inc=1, device_id={'pp': (stage + ds) % n_stage, 'tp': (z + dz) % n_tp}, device_id_type=MESH)
    pl.semaphore_wait(barrier, n_stage * n_tp - 1)

    for copy in w_copies[1]:
        copy.start()
    t_copy.start()

    @pl.when(stage == 0)
    def _():
        x_copy.wait()

    @pl.when(stage == last)
    def _():
        t_copy.wait()

    def flip():
        for src, dst in ((w1, w1t), (w2, w2t)):
            _, rows, columns = src.shape

            def tile_row(i, carry):
                k = i // (rows // TILE)
                at_row = pl.ds(pl.multiple_of((i % (rows // TILE)) * TILE, TILE), TILE)
                for j in range(columns // TILE):
                    js = pl.ds(j * TILE, TILE)
                    dst[k, js, at_row] = src[k, at_row, js].T
                return carry

            lax.fori_loop(0, 2 * (rows // TILE), tile_row, 0)

    @pl.when(stage > 0)
    def _():
        for pair in w_copies:
            for copy in pair:
                copy.wait()
        flip()

    def cols(c):
        return pl.ds(c * cw, cw)

    def part_send(p, slot, c):
        return pltpu.make_async_remote_copy(
            src_ref=part.at[p, slot, c], dst_ref=recv.at[center_i, p, slot, c],
            send_sem=part_sem.at[p, slot, c], recv_sem=recv_sem.at[center_i, p, slot, c],
            device_id={'pp': stage, 'tp': peer}, device_id_type=MESH)

    def part_arrival(kind, p, slot, c):
        return pltpu.make_async_remote_copy(
            src_ref=part.at[p, slot, c], dst_ref=recv.at[kind, p, slot, c],
            send_sem=part_sem.at[p, slot, c], recv_sem=recv_sem.at[kind, p, slot, c],
            device_id={'pp': stage, 'tp': peer}, device_id_type=MESH)

    def out_send(p, slot, c, q, m, to_stage, to_tp, sem):
        return pltpu.make_async_remote_copy(
            src_ref=outb.at[p, slot, c], dst_ref=xs.at[q, m, :, cols(c)],
            send_sem=sem.at[p, slot, c], recv_sem=x_sem.at[q, m, c],
            device_id={'pp': to_stage, 'tp': to_tp}, device_id_type=MESH)

    def at(v):
        fwd = (v >= 0) & (v < n)
        bwd = (v >= n + gap) & (v < 2 * n + gap)
        bwd_i = (v >= n).astype(jnp.int32)
        m = v - bwd_i * (n + gap)
        return fwd, bwd, bwd_i, m, m + bwd_i * n

    def arrived(q, m):
        for c in range(N_CHUNK):
            out_send(0, 0, c, q, m, stage, z, leaf_sem).wait_recv()

    def free_part(p, i):
        @pl.when(i >= SLOTS)
        def _():
            for c in range(N_CHUNK):
                part_send(p, i % SLOTS, c).wait_send()

    def send_part(p, slot, c):
        @pl.when(is_leaf)
        def _():
            part_send(p, slot, c).start()

    def compute(v, p):
        fwd, bwd, _, m, i = at(v)
        slot = i % SLOTS

        @pl.when(fwd)
        def _():
            @pl.when((m == 0) & (stage == 0))
            def _():
                w_copies[p][0].wait()
            if p == 0:
                @pl.when(stage > 0)
                def _():
                    arrived(0, m)
            else:
                @pl.when(is_leaf)
                def _():
                    arrived(1, m)
            free_part(p, i)
            for j in range(hid // BLOCK):
                js = pl.ds(j * BLOCK, BLOCK)
                pre = dot_nn(xs[p, m], w1[p, :, js]).astype(BF16)
                us[p, m, :, js] = pre
                act_now[:, js] = gelu_only(pre.astype(F32)).astype(BF16)

            @pl.when((m == 0) & (stage == 0))
            def _():
                w_copies[p][1].wait()
            for c in range(N_CHUNK):
                part[p, slot, c] = dot_nn(act_now[...], w2[p, :, cols(c)])
                send_part(p, slot, c)

        @pl.when(bwd)
        def _():
            k = 1 - p
            if p == 0:
                @pl.when(is_leaf | (stage < last))
                def _():
                    arrived(2, m)
            else:
                @pl.when(is_leaf)
                def _():
                    arrived(3, m)

            def outs():
                return (pltpu.make_async_copy(xs.at[k, m], h_out.at[k, m], copy_sem.at[p, 0]),
                        pltpu.make_async_copy(xs.at[2 + p, m], g_out.at[k, m], copy_sem.at[p, 1]),
                        pltpu.make_async_copy(acts.at[k, m], a_out.at[k, m], copy_sem.at[p, 2]),
                        pltpu.make_async_copy(us.at[k, m], e_out.at[k, m], copy_sem.at[p, 3]))

            @pl.when(m > 0)
            def _():
                for copy in outs():
                    copy.wait()
            for j in range(hid // BLOCK):
                js = pl.ds(j * BLOCK, BLOCK)
                grad = dot_nn(xs[2 + p, m], w2t[k, :, js])
                act, slope = gelu_parts(us[k, m, :, js].astype(F32))
                acts[k, m, :, js] = act.astype(BF16)
                err = (slope * grad).astype(BF16)
                us[k, m, :, js] = err
                act_now[:, js] = err

            def down():
                free_part(p, i)
                for c in range(N_CHUNK):
                    part[p, slot, c] = dot_nn(act_now[...], w1t[k, :, cols(c)])
                    send_part(p, slot, c)

            if p == 0:
                down()
            else:
                pl.when(stage > 0)(down)
            for copy in outs():
                copy.start()

    def sums(v, p):
        fwd, bwd, bwd_i, m, i = at(v)
        live = fwd | bwd if p == 0 else fwd | (bwd & (stage > 0))
        return live & is_center, fwd, bwd_i, m, i, i % SLOTS

    def add_leaf(v, p, chunks):
        live, _, _, _, _, slot = sums(v, p)

        @pl.when(live)
        def _():
            for c in chunks:
                part_arrival(0, p, slot, c).wait_recv()
                part[p, slot, c] = part[p, slot, c] + recv[0, p, slot, c]
                part_send(p, slot, c).start()

    def finish(v, p, chunks):
        live, fwd, bwd_i, m, i, slot = sums(v, p)
        if p == 0:
            to_stage, q = stage, 1 + 2 * bwd_i
        else:
            home = (1 - bwd_i) * at_last_i
            to_stage, q = stage + (1 - home) * (1 - 2 * bwd_i), 2 * bwd_i + 2 * home

        @pl.when(live)
        def _():
            @pl.when(i >= SLOTS)
            def _():
                for c in chunks:
                    out_send(p, slot, c, q, m, to_stage, partner, leaf_sem).wait_send()
            if p == 1:
                @pl.when((i >= SLOTS) & ((stage < last) | (i >= SLOTS + n)))
                def _():
                    for c in chunks:
                        out_send(p, slot, c, q, m, to_stage, z, peer_sem).wait_send()
            for c in chunks:
                part_arrival(1, p, slot, c).wait_recv()
                res = (xs[2 * bwd_i + p, m, :, cols(c)].astype(F32) + (part[p, slot, c] + recv[1, p, slot, c])).astype(BF16)
                if p == 0:
                    outb[p, slot, c] = res
                    xs[q, m, :, cols(c)] = res
                else:
                    @pl.when((stage < last) | (bwd_i == 1))
                    def _():
                        outb[p, slot, c] = res
                        out_send(p, slot, c, q, m, to_stage, z, peer_sem).start()

                    @pl.when((stage == last) & (bwd_i == 0))
                    def _():
                        diff = res.astype(F32) - tgt[m, :, cols(c)].astype(F32)
                        grad = (diff * norm).astype(BF16)
                        outb[p, slot, c] = grad
                        xs[q, m, :, cols(c)] = grad
                        sq = diff * diff
                        acc = loss_acc[...]
                        for r in range(unit // 8):
                            for b in range(cw // 128):
                                acc = acc + sq[r * 8:(r + 1) * 8, b * 128:(b + 1) * 128]
                        loss_acc[...] = acc
                out_send(p, slot, c, q, m, to_stage, partner, leaf_sem).start()

    def step(t, carry):
        @pl.when((stage == 0) & (t == n + GAP - 1))
        def _():
            flip()

        for kind, lag, p, chunks in ORDER:
            if kind == 'dot':
                compute(t - lag - p * (OUTER_LAG - lag) * (1 - center_i), p)
            elif kind == 'sum':
                add_leaf(t - lag, p, chunks)
            else:
                finish(t - lag, p, chunks)
        return carry

    lax.fori_loop(0, 2 * n + GAP + 3, step, 0)

    @pl.when(stage < last)
    def _():
        t_copy.wait()

    for p in range(2):
        for slot in range(SLOTS):
            for c in range(N_CHUNK):
                part_send(p, slot, c).wait_send()

                @pl.when(is_center)
                def _():
                    out_send(p, slot, c, 0, 0, stage, partner, leaf_sem).wait_send()
                    if p == 1:
                        out_send(p, slot, c, 0, 0, stage, z, peer_sem).wait_send()
        k = 1 - p
        pltpu.make_async_copy(xs.at[k, 0], h_out.at[k, 0], copy_sem.at[p, 0]).wait()
        pltpu.make_async_copy(xs.at[2 + p, 0], g_out.at[k, 0], copy_sem.at[p, 1]).wait()
        pltpu.make_async_copy(acts.at[k, 0], a_out.at[k, 0], copy_sem.at[p, 2]).wait()
        pltpu.make_async_copy(us.at[k, 0], e_out.at[k, 0], copy_sem.at[p, 3]).wait()

    def loss_send(idx, to_stage, to_tp):
        return pltpu.make_async_remote_copy(
            src_ref=loss_src, dst_ref=loss_dst, send_sem=loss_sem.at[idx], recv_sem=loss_got.at[0],
            device_id={'pp': to_stage, 'tp': to_tp}, device_id_type=MESH)

    sender = is_center & (stage == last)

    @pl.when(sender)
    def _():
        total = jnp.sum(loss_acc[...]) * 0.5 * norm
        value = jnp.full(loss_src.shape, total, F32)
        loss_src[...] = value
        loss_out[...] = value
        sends = [loss_send(2 * s + b, s, z if b else partner) for s in range(n_stage) for b in range(2) if not (s == last and b)]
        for send in sends:
            send.start()
        for send in sends:
            send.wait_send()

    @pl.when(is_leaf | (stage < last))
    def _():
        loss_send(0, stage, z).wait_recv()
        loss_out[...] = loss_dst[...]


def weight_grads(h_ref, e_ref, a_ref, g_ref, loss_ref, first_ref, second_ref, total_ref, turned):
    half, block = pl.program_id(0), pl.program_id(2)

    def over_tokens(left_ref, right_ref, out_ref):
        rows = out_ref.shape[1]

        @pl.when(block == 0)
        def _():
            for i in range(rows // TILE):
                turned[i * TILE:(i + 1) * TILE, :] = left_ref[0, :, i * TILE:(i + 1) * TILE].T

        out_ref[0] = dot_nn(turned[:rows, :], right_ref[0])

    @pl.when(half == 0)
    def _():
        total_ref[0] = jnp.max(loss_ref[...])
        over_tokens(h_ref, e_ref, first_ref)

    @pl.when(half == 1)
    def _():
        over_tokens(a_ref, g_ref, second_ref)


def solution(mesh):
    def stage_body(x_micro, targets, w_in, w_out):
        n_micro, n_token, width = x_micro.shape
        hid = w_in.shape[3]
        n = n_micro * n_token // UNIT
        norm = 1.0 / (n_micro * n_token * width)
        cw = width // N_CHUNK
        any_spec = pl.BlockSpec(memory_space=pl.ANY)
        h, g, a, e, loss = pl.pallas_call(
            functools.partial(pipe_kernel, norm),
            out_shape=(
                jax.ShapeDtypeStruct((2, n, UNIT, width), BF16),
                jax.ShapeDtypeStruct((2, n, UNIT, width), BF16),
                jax.ShapeDtypeStruct((2, n, UNIT, hid), BF16),
                jax.ShapeDtypeStruct((2, n, UNIT, hid), BF16),
                jax.ShapeDtypeStruct((8, 128), F32),
            ),
            in_specs=[any_spec] * 4,
            out_specs=(any_spec, any_spec, any_spec, any_spec, pl.BlockSpec(memory_space=pltpu.VMEM)),
            scratch_shapes=[
                pltpu.VMEM((2, width, hid), BF16),
                pltpu.VMEM((2, hid, width), BF16),
                pltpu.VMEM((2, hid, width), BF16),
                pltpu.VMEM((2, width, hid), BF16),
                pltpu.VMEM((4, n, UNIT, width), BF16),
                pltpu.VMEM((2, n, UNIT, hid), BF16),
                pltpu.VMEM((2, n, UNIT, hid), BF16),
                pltpu.VMEM((n, UNIT, width), BF16),
                pltpu.VMEM((UNIT, hid), BF16),
                pltpu.VMEM((2, SLOTS, N_CHUNK, UNIT, cw), F32),
                pltpu.VMEM((2, 2, SLOTS, N_CHUNK, UNIT, cw), F32),
                pltpu.VMEM((2, SLOTS, N_CHUNK, UNIT, cw), BF16),
                pltpu.VMEM((8, 128), F32),
                pltpu.VMEM((8, 128), F32),
                pltpu.VMEM((8, 128), F32),
                pltpu.SemaphoreType.DMA((2, 2)),
                pltpu.SemaphoreType.DMA((2,)),
                pltpu.SemaphoreType.DMA((4, n, N_CHUNK)),
                pltpu.SemaphoreType.DMA((2, SLOTS, N_CHUNK)),
                pltpu.SemaphoreType.DMA((2, 2, SLOTS, N_CHUNK)),
                pltpu.SemaphoreType.DMA((2, SLOTS, N_CHUNK)),
                pltpu.SemaphoreType.DMA((2, SLOTS, N_CHUNK)),
                pltpu.SemaphoreType.DMA((2, 4)),
                pltpu.SemaphoreType.DMA((8,)),
                pltpu.SemaphoreType.DMA((1,)),
            ],
            compiler_params=pltpu.CompilerParams(collective_id=0, has_side_effects=True, vmem_limit_bytes=67043328),
        )(x_micro.reshape(n, UNIT, width), targets.reshape(n, UNIT, width), w_in[0], w_out[0])

        h, g = (v.reshape(2, n * UNIT, width) for v in (h, g))
        a, e = (v.reshape(2, n * UNIT, hid) for v in (a, e))
        tokens = n * UNIT
        grad_first, grad_second, total = pl.pallas_call(
            weight_grads,
            grid=(2, 2, GRAD_BLOCKS),
            out_shape=(
                jax.ShapeDtypeStruct((2, width, hid), F32),
                jax.ShapeDtypeStruct((2, hid, width), F32),
                jax.ShapeDtypeStruct((1,), F32),
            ),
            in_specs=[
                pl.BlockSpec((1, tokens, width), lambda i, k, j: (k + i * (1 - k), 0, 0)),
                pl.BlockSpec((1, tokens, hid // GRAD_BLOCKS), lambda i, k, j: (k + i * (1 - k), 0, j + i * (GRAD_BLOCKS - 1 - j))),
                pl.BlockSpec((1, tokens, hid), lambda i, k, j: (k * i, 0, 0)),
                pl.BlockSpec((1, tokens, width // GRAD_BLOCKS), lambda i, k, j: (k * i, 0, j * i)),
                pl.BlockSpec(memory_space=pltpu.VMEM),
            ],
            out_specs=(
                pl.BlockSpec((1, width, hid // GRAD_BLOCKS), lambda i, k, j: (k + i * (1 - k), 0, j + i * (GRAD_BLOCKS - 1 - j))),
                pl.BlockSpec((1, hid, width // GRAD_BLOCKS), lambda i, k, j: (k * i, 0, j * i)),
                pl.BlockSpec(memory_space=pltpu.SMEM),
            ),
            scratch_shapes=[pltpu.VMEM((max(width, hid), tokens), BF16)],
            compiler_params=pltpu.CompilerParams(vmem_limit_bytes=56 * 1024 * 1024),
        )(h, e, a, g, loss)
        return grad_first[None], grad_second[None], total

    data_spec = P('dp', None, None)
    return jax.shard_map(stage_body, mesh=mesh, in_specs=(data_spec, data_spec, P('pp', None, None, 'tp'), P('pp', None, 'tp', None)), out_specs=(P(('dp', 'pp'), None, None, 'tp'), P(('dp', 'pp'), None, 'tp', None), P('dp')), check_vma=False)
```

```python
import functools
import math

import jax
import jax.numpy as jnp
from jax import lax
from jax.experimental import pallas as pl
from jax.experimental.pallas import tpu as pltpu
from jax.sharding import PartitionSpec as P

UNIT = 32
N_CHUNK = 3
SLOTS = 4
BLOCK = 512
GRAD_BLOCKS = 3
TILE = 256
GAP = 4

MESH = pl.DeviceIdType.MESH
F32 = jnp.float32
BF16 = jnp.bfloat16
ROOT = math.sqrt(2 / math.pi)
CUBIC = 0.044715


ALL = tuple(range(N_CHUNK))
ORDER = (('sum', 3, 1, (1,)), ('dot', 0, 0, ALL), ('sum', 3, 1, (2,)), ('end', 1, 0, (1, 0)), ('sum', 0, 0, (0, 1)), ('end', 1, 0, (2,)),
         ('dot', 1, 1, ALL), ('end', 3, 1, (0,)), ('sum', 0, 0, (2,)), ('end', 3, 1, (1,)), ('sum', 2, 1, (0,)), ('end', 3, 1, (2,)))
OUTER_LAG = 2


def gelu_parts(val):
    th = jnp.tanh(ROOT * (val + CUBIC * (val * val * val)))
    cdf = 0.5 * (1.0 + th)
    return val * cdf, cdf + val * (0.5 * (1.0 - th * th) * (ROOT * (1.0 + 3.0 * CUBIC * (val * val))))


def gelu_only(val):
    return val * (0.5 * (1.0 + jnp.tanh(ROOT * (val + CUBIC * (val * val * val)))))


def dot_nn(a, b):
    return jnp.dot(a, b, preferred_element_type=F32)


def pipe_kernel(norm, x_hbm, t_hbm, w1_hbm, w2_hbm,
                h_out, g_out, a_out, e_out, loss_out,
                w1, w2, w1t, w2t, xs, us, acts, tgt, act_now, part, recv, outb, loss_acc, loss_src, loss_dst,
                w_sem, in_sem, x_sem, part_sem, recv_sem, leaf_sem, peer_sem, copy_sem, loss_sem, loss_got):
    n_stage, n_tp = 4, 4
    _, n, unit, width = xs.shape
    hid = us.shape[3]
    cw = width // N_CHUNK
    stage = lax.axis_index('pp')
    z = lax.axis_index('tp')
    last = n_stage - 1
    is_center = (z == 1) | (z == 2)
    is_leaf = (z == 0) | (z == 3)
    center_i = is_center.astype(jnp.int32)
    partner = z + 1 - 2 * (z % 2)
    peer = partner + center_i * (3 - z - partner)
    at_last_i = (stage == last).astype(jnp.int32)
    gap = GAP * (1 - at_last_i)

    w_copies = []
    for k in range(2):
        w_copies.append((pltpu.make_async_copy(w1_hbm.at[k], w1.at[k], w_sem.at[0, k]),
                         pltpu.make_async_copy(w2_hbm.at[k], w2.at[k], w_sem.at[1, k])))
    x_copy = pltpu.make_async_copy(x_hbm, xs.at[0], in_sem.at[0])
    t_copy = pltpu.make_async_copy(t_hbm, tgt, in_sem.at[1])

    @pl.when(stage == 0)
    def _():
        x_copy.start()

    for copy in w_copies[0]:
        copy.start()
    loss_acc[...] = jnp.zeros_like(loss_acc)

    barrier = pltpu.get_barrier_semaphore()
    for ds in range(n_stage):
        for dz in range(n_tp):
            if ds or dz:
                pl.semaphore_signal(barrier, inc=1, device_id={'pp': (stage + ds) % n_stage, 'tp': (z + dz) % n_tp}, device_id_type=MESH)
    pl.semaphore_wait(barrier, n_stage * n_tp - 1)

    for copy in w_copies[1]:
        copy.start()
    t_copy.start()

    @pl.when(stage == 0)
    def _():
        x_copy.wait()

    @pl.when(stage == last)
    def _():
        t_copy.wait()

    def flip():
        for src, dst in ((w1, w1t), (w2, w2t)):
            _, rows, columns = src.shape

            def tile_row(i, carry):
                k = i // (rows // TILE)
                at_row = pl.ds(pl.multiple_of((i % (rows // TILE)) * TILE, TILE), TILE)
                for j in range(columns // TILE):
                    js = pl.ds(j * TILE, TILE)
                    dst[k, js, at_row] = src[k, at_row, js].T
                return carry

            lax.fori_loop(0, 2 * (rows // TILE), tile_row, 0)

    @pl.when(stage > 0)
    def _():
        for pair in w_copies:
            for copy in pair:
                copy.wait()
        flip()

    def cols(c):
        return pl.ds(c * cw, cw)

    def part_send(p, slot, c):
        return pltpu.make_async_remote_copy(
            src_ref=part.at[p, slot, c], dst_ref=recv.at[center_i, p, slot, c],
            send_sem=part_sem.at[p, slot, c], recv_sem=recv_sem.at[center_i, p, slot, c],
            device_id={'pp': stage, 'tp': peer}, device_id_type=MESH)

    def part_arrival(kind, p, slot, c):
        return pltpu.make_async_remote_copy(
            src_ref=part.at[p, slot, c], dst_ref=recv.at[kind, p, slot, c],
            send_sem=part_sem.at[p, slot, c], recv_sem=recv_sem.at[kind, p, slot, c],
            device_id={'pp': stage, 'tp': peer}, device_id_type=MESH)

    def out_send(p, slot, c, q, m, to_stage, to_tp, sem):
        return pltpu.make_async_remote_copy(
            src_ref=outb.at[p, slot, c], dst_ref=xs.at[q, m, :, cols(c)],
            send_sem=sem.at[p, slot, c], recv_sem=x_sem.at[q, m, c],
            device_id={'pp': to_stage, 'tp': to_tp}, device_id_type=MESH)

    def at(v):
        fwd = (v >= 0) & (v < n)
        bwd = (v >= n + gap) & (v < 2 * n + gap)
        bwd_i = (v >= n).astype(jnp.int32)
        m = v - bwd_i * (n + gap)
        return fwd, bwd, bwd_i, m, m + bwd_i * n

    def arrived(q, m):
        for c in range(N_CHUNK):
            out_send(0, 0, c, q, m, stage, z, leaf_sem).wait_recv()

    def free_part(p, i):
        @pl.when(i >= SLOTS)
        def _():
            for c in range(N_CHUNK):
                part_send(p, i % SLOTS, c).wait_send()

    def send_part(p, slot, c):
        @pl.when(is_leaf)
        def _():
            part_send(p, slot, c).start()

    def compute(v, p):
        fwd, bwd, _, m, i = at(v)
        slot = i % SLOTS

        @pl.when(fwd)
        def _():
            @pl.when((m == 0) & (stage == 0))
            def _():
                w_copies[p][0].wait()
            if p == 0:
                @pl.when(stage > 0)
                def _():
                    arrived(0, m)
            else:
                @pl.when(is_leaf)
                def _():
                    arrived(1, m)
            free_part(p, i)
            for j in range(hid // BLOCK):
                js = pl.ds(j * BLOCK, BLOCK)
                pre = dot_nn(xs[p, m], w1[p, :, js]).astype(BF16)
                us[p, m, :, js] = pre
                act_now[:, js] = gelu_only(pre.astype(F32)).astype(BF16)

            @pl.when((m == 0) & (stage == 0))
            def _():
                w_copies[p][1].wait()
            for c in range(N_CHUNK):
                part[p, slot, c] = dot_nn(act_now[...], w2[p, :, cols(c)])
                send_part(p, slot, c)

        @pl.when(bwd)
        def _():
            k = 1 - p
            if p == 0:
                @pl.when(is_leaf | (stage < last))
                def _():
                    arrived(2, m)
            else:
                @pl.when(is_leaf)
                def _():
                    arrived(3, m)

            def outs():
                return (pltpu.make_async_copy(xs.at[k, m], h_out.at[k, m], copy_sem.at[p, 0]),
                        pltpu.make_async_copy(xs.at[2 + p, m], g_out.at[k, m], copy_sem.at[p, 1]),
                        pltpu.make_async_copy(acts.at[k, m], a_out.at[k, m], copy_sem.at[p, 2]),
                        pltpu.make_async_copy(us.at[k, m], e_out.at[k, m], copy_sem.at[p, 3]))

            @pl.when(m > 0)
            def _():
                for copy in outs():
                    copy.wait()
            for j in range(hid // BLOCK):
                js = pl.ds(j * BLOCK, BLOCK)
                grad = dot_nn(xs[2 + p, m], w2t[k, :, js])
                act, slope = gelu_parts(us[k, m, :, js].astype(F32))
                acts[k, m, :, js] = act.astype(BF16)
                err = (slope * grad).astype(BF16)
                us[k, m, :, js] = err
                act_now[:, js] = err

            def down():
                free_part(p, i)
                for c in range(N_CHUNK):
                    part[p, slot, c] = dot_nn(act_now[...], w1t[k, :, cols(c)])
                    send_part(p, slot, c)

            if p == 0:
                down()
            else:
                pl.when(stage > 0)(down)
            for copy in outs():
                copy.start()

    def sums(v, p):
        fwd, bwd, bwd_i, m, i = at(v)
        live = fwd | bwd if p == 0 else fwd | (bwd & (stage > 0))
        return live & is_center, fwd, bwd_i, m, i, i % SLOTS

    def add_leaf(v, p, chunks):
        live, _, _, _, _, slot = sums(v, p)

        @pl.when(live)
        def _():
            for c in chunks:
                part_arrival(0, p, slot, c).wait_recv()
                part[p, slot, c] = part[p, slot, c] + recv[0, p, slot, c]
                part_send(p, slot, c).start()

    def finish(v, p, chunks):
        live, fwd, bwd_i, m, i, slot = sums(v, p)
        if p == 0:
            to_stage, q = stage, 1 + 2 * bwd_i
        else:
            home = (1 - bwd_i) * at_last_i
            to_stage, q = stage + (1 - home) * (1 - 2 * bwd_i), 2 * bwd_i + 2 * home

        @pl.when(live)
        def _():
            @pl.when(i >= SLOTS)
            def _():
                for c in chunks:
                    out_send(p, slot, c, q, m, to_stage, partner, leaf_sem).wait_send()
            if p == 1:
                @pl.when((i >= SLOTS) & ((stage < last) | (i >= SLOTS + n)))
                def _():
                    for c in chunks:
                        out_send(p, slot, c, q, m, to_stage, z, peer_sem).wait_send()
            for c in chunks:
                part_arrival(1, p, slot, c).wait_recv()
                res = (xs[2 * bwd_i + p, m, :, cols(c)].astype(F32) + (part[p, slot, c] + recv[1, p, slot, c])).astype(BF16)
                if p == 0:
                    outb[p, slot, c] = res
                    xs[q, m, :, cols(c)] = res
                else:
                    @pl.when((stage < last) | (bwd_i == 1))
                    def _():
                        outb[p, slot, c] = res
                        out_send(p, slot, c, q, m, to_stage, z, peer_sem).start()

                    @pl.when((stage == last) & (bwd_i == 0))
                    def _():
                        diff = res.astype(F32) - tgt[m, :, cols(c)].astype(F32)
                        grad = (diff * norm).astype(BF16)
                        outb[p, slot, c] = grad
                        xs[q, m, :, cols(c)] = grad
                        sq = diff * diff
                        acc = loss_acc[...]
                        for r in range(unit // 8):
                            for b in range(cw // 128):
                                acc = acc + sq[r * 8:(r + 1) * 8, b * 128:(b + 1) * 128]
                        loss_acc[...] = acc
                out_send(p, slot, c, q, m, to_stage, partner, leaf_sem).start()

    def step(t, carry):
        @pl.when((stage == 0) & (t == n + GAP - 1))
        def _():
            flip()

        for kind, lag, p, chunks in ORDER:
            if kind == 'dot':
                compute(t - lag - p * (OUTER_LAG - lag) * (1 - center_i), p)
            elif kind == 'sum':
                add_leaf(t - lag, p, chunks)
            else:
                finish(t - lag, p, chunks)
        return carry

    lax.fori_loop(0, 2 * n + GAP + 3, step, 0)

    @pl.when(stage < last)
    def _():
        t_copy.wait()

    for p in range(2):
        for slot in range(SLOTS):
            for c in range(N_CHUNK):
                part_send(p, slot, c).wait_send()

                @pl.when(is_center)
                def _():
                    out_send(p, slot, c, 0, 0, stage, partner, leaf_sem).wait_send()
                    if p == 1:
                        out_send(p, slot, c, 0, 0, stage, z, peer_sem).wait_send()
        k = 1 - p
        pltpu.make_async_copy(xs.at[k, 0], h_out.at[k, 0], copy_sem.at[p, 0]).wait()
        pltpu.make_async_copy(xs.at[2 + p, 0], g_out.at[k, 0], copy_sem.at[p, 1]).wait()
        pltpu.make_async_copy(acts.at[k, 0], a_out.at[k, 0], copy_sem.at[p, 2]).wait()
        pltpu.make_async_copy(us.at[k, 0], e_out.at[k, 0], copy_sem.at[p, 3]).wait()

    def loss_send(idx, to_stage, to_tp):
        return pltpu.make_async_remote_copy(
            src_ref=loss_src, dst_ref=loss_dst, send_sem=loss_sem.at[idx], recv_sem=loss_got.at[0],
            device_id={'pp': to_stage, 'tp': to_tp}, device_id_type=MESH)

    sender = is_center & (stage == last)

    @pl.when(sender)
    def _():
        total = jnp.sum(loss_acc[...]) * 0.5 * norm
        value = jnp.full(loss_src.shape, total, F32)
        loss_src[...] = value
        loss_out[...] = value
        sends = [loss_send(2 * s + b, s, z if b else partner) for s in range(n_stage) for b in range(2) if not (s == last and b)]
        for send in sends:
            send.start()
        for send in sends:
            send.wait_send()

    @pl.when(is_leaf | (stage < last))
    def _():
        loss_send(0, stage, z).wait_recv()
        loss_out[...] = loss_dst[...]


def weight_grads(h_hbm, e_hbm, a_hbm, g_hbm, loss_ref, first_hbm, second_hbm, total_ref, lefts, rights, firsts, seconds, turned, in_sem, out_sem):
    total_ref[0] = jnp.max(loss_ref[...])
    jobs = []
    for k in range(2):
        jobs.append((0, k, h_hbm, e_hbm, firsts, first_hbm))
        jobs.append((1, k, a_hbm, g_hbm, seconds, second_hbm))

    def loads(job):
        kind, k, left, right, _, _ = job
        rows, columns = left.shape[2], right.shape[2]
        return (pltpu.make_async_copy(left.at[k], lefts.at[kind, k, :, pl.ds(0, rows)], in_sem.at[kind, k, 0]),
                pltpu.make_async_copy(right.at[k], rights.at[kind, k, :, pl.ds(0, columns)], in_sem.at[kind, k, 1]))

    def store(job, j):
        kind, k, _, _, result, out = job
        width = out.shape[2] // GRAD_BLOCKS
        return pltpu.make_async_copy(result.at[k, j], out.at[k, :, pl.ds(j * width, width)], out_sem.at[kind, k, j])

    for copy in loads(jobs[0]):
        copy.start()
    for number, job in enumerate(jobs):
        kind, k, left, right, result, out = job
        rows, width = left.shape[2], right.shape[2] // GRAD_BLOCKS
        for copy in loads(job):
            copy.wait()
        if number == 0:
            for other in jobs[1:]:
                for copy in loads(other):
                    copy.start()
        for i in range(rows // TILE):
            turned[i * TILE:(i + 1) * TILE, :] = lefts[kind, k, :, i * TILE:(i + 1) * TILE].T
        for j in range(GRAD_BLOCKS):
            result[k, j] = dot_nn(turned[:rows, :], rights[kind, k, :, j * width:(j + 1) * width])
            store(job, j).start()
    for job in jobs:
        for j in range(GRAD_BLOCKS):
            store(job, j).wait()


def solution(mesh):
    def stage_body(x_micro, targets, w_in, w_out):
        n_micro, n_token, width = x_micro.shape
        hid = w_in.shape[3]
        n = n_micro * n_token // UNIT
        norm = 1.0 / (n_micro * n_token * width)
        cw = width // N_CHUNK
        any_spec = pl.BlockSpec(memory_space=pl.ANY)
        h, g, a, e, loss = pl.pallas_call(
            functools.partial(pipe_kernel, norm),
            out_shape=(
                jax.ShapeDtypeStruct((2, n, UNIT, width), BF16),
                jax.ShapeDtypeStruct((2, n, UNIT, width), BF16),
                jax.ShapeDtypeStruct((2, n, UNIT, hid), BF16),
                jax.ShapeDtypeStruct((2, n, UNIT, hid), BF16),
                jax.ShapeDtypeStruct((8, 128), F32),
            ),
            in_specs=[any_spec] * 4,
            out_specs=(any_spec, any_spec, any_spec, any_spec, pl.BlockSpec(memory_space=pltpu.VMEM)),
            scratch_shapes=[
                pltpu.VMEM((2, width, hid), BF16),
                pltpu.VMEM((2, hid, width), BF16),
                pltpu.VMEM((2, hid, width), BF16),
                pltpu.VMEM((2, width, hid), BF16),
                pltpu.VMEM((4, n, UNIT, width), BF16),
                pltpu.VMEM((2, n, UNIT, hid), BF16),
                pltpu.VMEM((2, n, UNIT, hid), BF16),
                pltpu.VMEM((n, UNIT, width), BF16),
                pltpu.VMEM((UNIT, hid), BF16),
                pltpu.VMEM((2, SLOTS, N_CHUNK, UNIT, cw), F32),
                pltpu.VMEM((2, 2, SLOTS, N_CHUNK, UNIT, cw), F32),
                pltpu.VMEM((2, SLOTS, N_CHUNK, UNIT, cw), BF16),
                pltpu.VMEM((8, 128), F32),
                pltpu.VMEM((8, 128), F32),
                pltpu.VMEM((8, 128), F32),
                pltpu.SemaphoreType.DMA((2, 2)),
                pltpu.SemaphoreType.DMA((2,)),
                pltpu.SemaphoreType.DMA((4, n, N_CHUNK)),
                pltpu.SemaphoreType.DMA((2, SLOTS, N_CHUNK)),
                pltpu.SemaphoreType.DMA((2, 2, SLOTS, N_CHUNK)),
                pltpu.SemaphoreType.DMA((2, SLOTS, N_CHUNK)),
                pltpu.SemaphoreType.DMA((2, SLOTS, N_CHUNK)),
                pltpu.SemaphoreType.DMA((2, 4)),
                pltpu.SemaphoreType.DMA((8,)),
                pltpu.SemaphoreType.DMA((1,)),
            ],
            compiler_params=pltpu.CompilerParams(collective_id=0, has_side_effects=True, vmem_limit_bytes=67043328),
        )(x_micro.reshape(n, UNIT, width), targets.reshape(n, UNIT, width), w_in[0], w_out[0])

        h, g = (v.reshape(2, n * UNIT, width) for v in (h, g))
        a, e = (v.reshape(2, n * UNIT, hid) for v in (a, e))
        tokens = n * UNIT
        grad_first, grad_second, total = pl.pallas_call(
            weight_grads,
            out_shape=(
                jax.ShapeDtypeStruct((2, width, hid), F32),
                jax.ShapeDtypeStruct((2, hid, width), F32),
                jax.ShapeDtypeStruct((1,), F32),
            ),
            in_specs=[any_spec] * 4 + [pl.BlockSpec(memory_space=pltpu.VMEM)],
            out_specs=(any_spec, any_spec, pl.BlockSpec(memory_space=pltpu.SMEM)),
            scratch_shapes=[
                pltpu.VMEM((2, 2, tokens, max(width, hid)), BF16),
                pltpu.VMEM((2, 2, tokens, max(width, hid)), BF16),
                pltpu.VMEM((2, GRAD_BLOCKS, width, hid // GRAD_BLOCKS), F32),
                pltpu.VMEM((2, GRAD_BLOCKS, hid, width // GRAD_BLOCKS), F32),
                pltpu.VMEM((max(width, hid), tokens), BF16),
                pltpu.SemaphoreType.DMA((2, 2, 2)),
                pltpu.SemaphoreType.DMA((2, 2, GRAD_BLOCKS)),
            ],
            compiler_params=pltpu.CompilerParams(vmem_limit_bytes=67043328),
        )(h, e, a, g, loss)
        return grad_first[None], grad_second[None], total

    data_spec = P('dp', None, None)
    return jax.shard_map(stage_body, mesh=mesh, in_specs=(data_spec, data_spec, P('pp', None, None, 'tp'), P('pp', None, 'tp', None)), out_specs=(P(('dp', 'pp'), None, None, 'tp'), P(('dp', 'pp'), None, 'tp', None), P('dp')), check_vma=False)
```
